32 devices in a mesh: row: 4 (over y, core), col: 4 (over z), depth: 2 (over x).
Axes of the slice: x: 2, y: 2, z: 4, core: 2. Of those that a mesh axis runs over, the one named last changes fastest.
Arguments:
- diag_block: float32 [512, 512], P(('row', 'col', 'depth')), as said below
- panel_rows: float32 [32256, 512], P(('row', 'col', 'depth')), may hold values from -2 to 2
- trailing: float32 [32256, 1024], P(('row', 'depth'), 'col'), may hold values from -6 to 6
Outputs:
- diag_factor: float32 [512, 512], P(('row', 'col', 'depth'))
- panel_factor: float32 [32256, 512], P(('row', 'col', 'depth'))
- updated: float32 [32256, 1024], P(('row', 'depth'), 'col')
The draws below stay inside these ranges and needn't reach their ends.
Inputs may be any that keep to these rules, and one draw needn't show every extreme that they name: `diag_block`: symmetric positive definite.
All inputs are finite; a program needn't handle non-finite values.
Results may differ from the reference program's by a relative error of at most 0.000062.
Values sent between devices are 32-bit elements; how exact they have to be, the bound alone decides.
A program may use at most 64 MiB of HBM per device.

```python
import math
import jax
import jax.numpy as jnp
from jax import lax

PANEL = 512
WIN = 1024
TRAIL = 32256


def draw_diag_block(key, part):
    first = jax.random.fold_in(key, 11)
    second = jax.random.fold_in(key, 12)
    noise = jax.random.normal(first, (PANEL, PANEL), jnp.float32)
    sym = (noise + noise.T) / math.sqrt(2.0 * PANEL)
    shift = jax.random.uniform(second, (PANEL,), jnp.float32, 3.0, 6.0)
    matrix = sym + jnp.diag(shift)
    return matrix


def block_scale(own_key, dims, shards, low, high):
    factor_of = 1.0
    for position, shards_of in shards:
        draws = jax.random.uniform(jax.random.fold_in(jax.random.fold_in(own_key, 6), position), (shards_of,), jnp.float32, low / len(shards), high / len(shards))
        factor_of = factor_of * jnp.repeat(jnp.exp(draws), dims[position] // shards_of).reshape((-1,) + (1,) * (len(dims) - 1 - position))
    return factor_of


def scatter_about(own_key, extent, scale, reach, shards=(), kind=jnp.bfloat16):
    gain = block_scale(own_key, extent, shards, -0.22, 0.18) if shards else 1.0
    result = jax.random.normal(own_key, extent, jnp.float32) * scale * gain
    return jnp.minimum(jnp.maximum(result, -reach), reach).astype(kind)


def setup_inputs(seed: int = 0) -> dict:
    seeds = jax.random.split(jax.random.key(seed), 4)
    diag_block = draw_diag_block(jax.random.fold_in(seeds[3], 71), 0)
    panel_rows = scatter_about(seeds[1], (TRAIL, PANEL), 0.25, 2.0, ((0, 32),), jnp.float32)
    trailing = scatter_about(seeds[2], (TRAIL, WIN), 1.0, 6.0, ((0, 8), (1, 4)), jnp.float32)
    return {"diag_block": diag_block, "panel_rows": panel_rows, "trailing": trailing}


def reference(diag_block, panel_rows, trailing):
    diag_factor = jnp.linalg.cholesky(diag_block)
    panel_factor = jax.scipy.linalg.solve_triangular(diag_factor, panel_rows.T, lower=True).T
    window = panel_factor[:trailing.shape[1]]
    product = lax.dot_general(panel_factor.astype(jnp.float32), window.astype(jnp.float32), (((1,), (1,)), ((), ())), precision=lax.Precision.HIGHEST, preferred_element_type=jnp.float32)
    return (diag_factor, panel_factor, trailing - product)
```

```python
import functools
import math

import jax
import jax.numpy as jnp
from jax import lax
from jax.experimental import pallas as pl
from jax.experimental.pallas import tpu as pltpu
from jax.sharding import PartitionSpec as P

highest = lax.Precision.HIGHEST
AXES = ("row", "col", "depth")
LANES = 128


def dot(left, right, left_dim, right_dim):
    return lax.dot_general(
        left, right, (((left_dim,), (right_dim,)), ((), ())), precision=highest, preferred_element_type=jnp.float32
    )


def factor_block(block, halfway=None):
    size = block.shape[0]
    lane = lax.broadcasted_iota(jnp.int32, (8, size), 1)
    sub = lax.broadcasted_iota(jnp.int32, (8, size), 0)
    tiles = [block[8 * i : 8 * i + 8, :] for i in range(size // 8)]
    for j in range(size):
        if halfway is not None and j == size // 2:
            halfway()
        t, s = divmod(j, 8)
        row = tiles[t][s : s + 1, :]
        inverse = 1.0 / row[:, j : j + 1]
        source = jnp.where(lane[0:1] == j, 1.0, row) * inverse
        for i in range(t, size // 8):
            if i == t and s == 7:
                continue
            tile = tiles[i]
            new = jnp.where(lane == j, 0.0, tile) - tile[:, j : j + 1] * source
            tiles[i] = jnp.where(sub > s, new, tile) if i == t else new
    whole = jnp.concatenate(tiles, axis=0)
    r_id = lax.broadcasted_iota(jnp.int32, (size, size), 0)
    c_id = lax.broadcasted_iota(jnp.int32, (size, size), 1)
    pivots = jnp.sum(jnp.where(r_id == c_id, whole, 0.0), axis=1, keepdims=True)
    root = jnp.sqrt(pivots)
    scaled = jnp.where(r_id == c_id, 1.0, whole) / root
    inverse = jnp.where(r_id >= c_id, scaled, 0.0)
    upper = jnp.where(r_id < c_id, scaled, jnp.where(r_id == c_id, root, 0.0))
    return upper.T, inverse


def factor_all(work, low, inv, between=None):
    n = work.shape[0]
    low[...] = jnp.zeros((n, n), jnp.float32)
    inv[...] = jnp.zeros((n, n), jnp.float32)

    def step(k, carry):
        at = pl.ds(pl.multiple_of(k * LANES, LANES), LANES)
        halfway = None if between is None else functools.partial(between, k, 0)
        block_low, block_inv = factor_block(work[at, at], halfway)
        rows = lax.broadcasted_iota(jnp.int32, (n, LANES), 0)
        panel = jnp.where(rows >= (k + 1) * LANES, dot(work[:, at], block_inv, 1, 1), 0.0)
        work[...] = work[...] - dot(panel, panel, 1, 1)
        left = dot(low[at, :], inv[...], 1, 0)
        low[:, at] = panel
        low[at, at] = block_low
        inv[at, :] = -dot(block_inv, left, 1, 0)
        inv[at, at] = block_inv
        if between is not None:
            between(k, 1)
        return carry

    lax.fori_loop(0, n // LANES, step, 0)


def exchange(sizes, cuts, win_units, diag_ref, panel, low, weight, solved, held, window, pieces, work, inv, sems):
    n_r, n_c, n_d = sizes
    total = n_r * n_c * n_d
    half = n_c // 2
    units = panel.shape[0]
    (diag_s, diag_r, ring_s, ring_r, deep_s, deep_r, w1_s, w1_r, w2_s, w2_r, w3_s, w3_r, own_s) = sems
    r, c, d = lax.axis_index("row"), lax.axis_index("col"), lax.axis_index("depth")
    position = (r * n_c + c) * n_d + d

    def remote(src, dst, send, recv, **where):
        return pltpu.make_async_remote_copy(
            src_ref=src,
            dst_ref=dst,
            send_sem=send,
            recv_sem=recv,
            device_id={"row": where.get("row", r), "col": where.get("col", c), "depth": where.get("depth", d)},
            device_id_type=pl.DeviceIdType.MESH,
        )

    def taker(block):
        return lax.div(block * n_d + d, n_c)

    def slot(block):
        return jnp.where(taker(block) == d, block * n_d + d - n_c * d, n_c + block)

    def at(h):
        return pl.ds(cuts[h], cuts[h + 1] - cuts[h])

    def send_diag(k, carry):
        to = lax.rem(position + k, total)
        remote(
            diag_ref, pieces.at[position], diag_s, diag_r,
            row=lax.div(to, n_c * n_d), col=lax.rem(lax.div(to, n_d), n_c), depth=lax.rem(to, n_d),
        ).start()
        return carry

    lax.fori_loop(1, total, send_diag, 0)
    pieces[position] = diag_ref[...]

    def window_parts():
        for p in range(-(-n_c * win_units // units)):
            for b in range(n_c):
                lo, hi = max(b * win_units, p * units), min((b + 1) * win_units, (p + 1) * units)
                if lo < hi:
                    yield p, b, lo, hi - lo

    def part(p, b, lo, count):
        src = panel.at[pl.ds(lo - p * units, count)]
        dst = window.at[pl.ds(lo - b * win_units, count)]
        if p == b * n_d:
            return pltpu.make_async_copy(src, dst, w1_r.at[p])
        return remote(src, dst, w1_s.at[p, b], w1_r.at[p], row=0, col=b, depth=0)

    root = jnp.logical_and(r == 0, d == 0)
    for p, b, lo, count in window_parts():
        @pl.when(position == p)
        def _(p=p, b=b, lo=lo, count=count):
            part(p, b, lo, count).start()

    def to_depth(k):
        return remote(window, window, w2_s.at[k], w2_r, depth=k)

    def to_row(k):
        return remote(window, window, w3_s.at[k], w3_r, row=k)

    def window_second():
        for p, b, lo, count in window_parts():
            @pl.when(jnp.logical_and(root, c == b))
            def _(p=p, b=b, lo=lo, count=count):
                if p == b * n_d:
                    part(p, b, lo, count).wait()
                else:
                    piece = window.at[pl.ds(lo - b * win_units, count)]
                    pltpu.make_async_copy(piece, piece, w1_r.at[p]).wait()

        @pl.when(root)
        def _():
            for k in range(1, n_d):
                to_depth(k).start()

    def window_third():
        @pl.when(jnp.logical_and(r == 0, d != 0))
        def _():
            pltpu.make_async_copy(window, window, w2_r).wait()

        @pl.when(r == 0)
        def _():
            for k in range(1, n_r):
                to_row(k).start()

    def ring(way, s, h):
        block = lax.rem(c + n_c - s + 1, n_c) if way == 0 else lax.rem(c + s - 1, n_c)
        to = lax.rem(c + 1, n_c) if way == 0 else lax.rem(c + n_c - 1, n_c)
        dst = held.at[slot(block), at(h)]
        src = panel.at[at(h)] if s == 1 else dst
        return remote(src, dst, ring_s.at[way, s - 1, h], ring_r.at[way, s - 1, h], col=to)

    def ring_parts(s):
        return [(0, 0), (1, 1)] + ([(0, 1), (1, 0)] if s < half else [])

    def deep(step, h):
        block = lax.rem(c + n_c - step, n_c)
        to = taker(block)
        index = block * n_d + d - n_c * to
        src = panel.at[at(h)] if step == 0 else held.at[slot(block), at(h)]
        where = step + half - 1
        return to, remote(
            src, held.at[index, at(h)], deep_s.at[where, h], deep_r.at[index, h], depth=to
        )

    def start_deep(step, h):
        to, copy = deep(step, h)

        @pl.when(to != d)
        def _():
            copy.start()

    def own_copy():
        return pltpu.make_async_copy(panel, held.at[slot(c)], own_s)

    for way, h in ring_parts(1):
        ring(way, 1, h).start()
    for h in range(2):
        start_deep(0, h)

    @pl.when(taker(c) == d)
    def _():
        own_copy().start()

    def arrived(s, parts):
        for way, h in parts:
            ring(way, s, h).wait_recv()
            if s < half and (s + 1 < half or way == h):
                ring(way, s + 1, h).start()
            step = s if (way == 0 or s == half) else -s
            start_deep(step, h)

    def between(k, later):
        def when(point, action):
            if point % 2 == later:
                pl.when(k == point // 2)(action)

        when(1, window_second)
        when(3, window_third)
        if half > 1:
            when(2, lambda: arrived(1, ring_parts(1)[:2]))
            when(6, lambda: arrived(1, ring_parts(1)[2:]))

    every = pieces.at[pl.ds(0, total - 1)]
    pltpu.make_async_copy(every, every, diag_r).wait()
    mine = diag_ref.shape[0]
    for p in range(total):
        work[p * mine : (p + 1) * mine, :] = pieces[p]
    factor_all(work, low, inv, between)

    @pl.when(r != 0)
    def _():
        pltpu.make_async_copy(window, window, w3_r).wait()

    weight[...] = dot(dot(window[...].reshape(weight.shape), inv[...], 1, 1), inv[...], 1, 0)
    solved[...] = dot(panel[...].reshape(solved.shape), inv[...], 1, 1)
    for s in range(2 if half > 1 else 1, half + 1):
        arrived(s, ring_parts(s))

    for j in range(n_c):
        q = n_c * d + j

        @pl.when(lax.rem(q, n_d) != d)
        def _(j=j):
            for h in range(2):
                landed = held.at[j, at(h)]
                pltpu.make_async_copy(landed, landed, deep_r.at[j, h]).wait()

    pltpu.make_async_copy(every, every, diag_s).wait()
    for s in range(1, half + 1):
        for way, h in ring_parts(s):
            ring(way, s, h).wait_send()
    for step in range(1 - half, half + 1):
        for h in range(2):
            to, copy = deep(step, h)

            @pl.when(to != d)
            def _(copy=copy):
                copy.wait_send()

    @pl.when(taker(c) == d)
    def _():
        own_copy().wait()

    for p, b, lo, count in window_parts():
        if p != b * n_d:
            @pl.when(position == p)
            def _(p=p, b=b, lo=lo, count=count):
                part(p, b, lo, count).wait_send()

    @pl.when(root)
    def _():
        for k in range(1, n_d):
            to_depth(k).wait_send()

    @pl.when(r == 0)
    def _():
        for k in range(1, n_r):
            to_row(k).wait_send()


def exchange_call(sizes, diag_block, panel, win_units):
    n_r, n_c, n_d = sizes
    total = n_r * n_c * n_d
    units, unit, width = panel.shape
    n = diag_block.shape[1]
    square = jax.ShapeDtypeStruct((n, n), jnp.float32)
    vmem, anywhere = pl.BlockSpec(memory_space=pltpu.VMEM), pl.BlockSpec(memory_space=pl.ANY)
    dma, owners = pltpu.SemaphoreType.DMA, -(-n_c * win_units // units)
    sems = [
        dma, dma, dma((2, n_c // 2, 2)), dma((2, n_c // 2, 2)), dma((n_c, 2)), dma((n_c, 2)),
        dma((owners, n_c)), dma((owners,)), dma((n_d,)), dma, dma((n_r,)), dma, dma,
    ]
    return pl.pallas_call(
        functools.partial(exchange, sizes, (0, units // 2, units), win_units),
        out_shape=(
            square,
            jax.ShapeDtypeStruct((win_units * unit, width), jnp.float32),
            jax.ShapeDtypeStruct((units * unit, width), jnp.float32),
            jax.ShapeDtypeStruct((2 * n_c, units, unit, width), jnp.float32),
        ),
        in_specs=[vmem, vmem],
        out_specs=(vmem, vmem, vmem, anywhere),
        scratch_shapes=[
            pltpu.VMEM((win_units, unit, width), jnp.float32),
            pltpu.VMEM((total, diag_block.shape[0], n), jnp.float32),
            pltpu.VMEM((n, n), jnp.float32),
            pltpu.VMEM((n, n), jnp.float32),
            sems,
        ],
        compiler_params=pltpu.CompilerParams(has_side_effects=True),
    )(diag_block, panel)


def update(held, weight, trailing, out):
    out[...] = trailing[...] - dot(held[...], weight[...], 1, 1)


def update_call(held, weight, trailing):
    rows, columns = trailing.shape
    width = held.shape[1]
    chunk = max(m for m in range(8, 1025, 8) if rows % m == 0)
    return pl.pallas_call(
        update,
        grid=(rows // chunk,),
        out_shape=jax.ShapeDtypeStruct(trailing.shape, jnp.float32),
        in_specs=[
            pl.BlockSpec((chunk, width), lambda i: (i, 0)),
            pl.BlockSpec((columns, width), lambda i: (0, 0)),
            pl.BlockSpec((chunk, columns), lambda i: (i, 0)),
        ],
        out_specs=pl.BlockSpec((chunk, columns), lambda i: (i, 0)),
    )(held, weight, trailing)


def near(sizes, parts, split, diag_ref, panel, trailing, own, solved_out, updated, raw, wraw, mult, trail, solved, sent,
         landed, pieces, work, low, inv, dense, sems):
    n_r, n_c, n_d = sizes
    total = n_r * n_c * n_d
    planes = n_r // 2 * n_d
    last = n_c - 1
    per = n_c // n_d
    rows = raw.shape[1]
    size = rows // split
    (own_s, trail_s, piece_s, dz_s, dz_r, dp_s, dp_r, dc_s, dc_r, raw_s, raw_r, w1_s, w1_r, w2_s, w2_r, w3_s, w3_r, w4_s, w4_r,
     prod_s, prod_r, out_s, solved_s) = sems
    r, c, d = lax.axis_index("row"), lax.axis_index("col"), lax.axis_index("depth")
    y, core = lax.div(r, 2), lax.rem(r, 2)
    plane = y * n_d + d
    position = (r * n_c + c) * n_d + d

    def remote(src, dst, send, recv, **where):
        return pltpu.make_async_remote_copy(
            src_ref=src,
            dst_ref=dst,
            send_sem=send,
            recv_sem=recv,
            device_id={"row": where.get("row", r), "col": where.get("col", c), "depth": where.get("depth", d)},
            device_id_type=pl.DeviceIdType.MESH,
        )

    def at(h):
        return pl.ds(pl.multiple_of(h * size, 8), size)

    def landing(ref, sem):
        pltpu.make_async_copy(ref, ref, sem).wait()

    def diag_z(k):
        return remote(diag_ref, pieces.at[core, plane, c], dz_s.at[k], dz_r, col=lax.rem(c + k, n_c))

    def diag_plane(k):
        to = lax.rem(plane + k, planes)
        mine = pieces.at[core, plane]
        return remote(mine, mine, dp_s.at[k], dp_r, row=lax.div(to, n_d) * 2 + core, depth=lax.rem(to, n_d))

    def diag_core():
        return remote(pieces.at[core], pieces.at[core], dc_s, dc_r, row=y * 2 + 1 - core)

    takes = lax.div(c, per)
    goes = (c < last, c > 0, takes != d)
    comes = (c > 0, c < last, takes == d)
    steps = ({"col": c + 1}, {"col": c - 1}, {"depth": 1 - d})

    def raw_copy(way, h):
        return remote(raw.at[0, at(h)], raw.at[way + 1, at(h)], raw_s.at[way, h], raw_r.at[way, h], **steps[way])

    def raw_start(ways, hs):
        for h in hs:
            for way in ways:
                pl.when(goes[way])(lambda way=way, h=h: raw_copy(way, h).start())

    def first_targets(b):
        return [b] + ([q for q in range(planes) if q != b] if b == 0 else [])

    def first(i, q):
        p, b, lo, skip, count = parts[i]
        src, dst = raw.at[0, pl.ds(lo, count)], wraw.at[b, pl.ds(skip, count)]
        if p == (q // n_d * 2 * n_c) * n_d + q % n_d:
            return pltpu.make_async_copy(src, dst, w1_r.at[i])
        return remote(src, dst, w1_s.at[i, q], w1_r.at[i], row=q // n_d * 2, col=0, depth=q % n_d)

    def first_start():
        for late in (False, True):
            for i, (p, b, lo, skip, count) in enumerate(parts):
                for q in first_targets(b):
                    if (q != b) == late:
                        pl.when(position == p)(lambda i=i, q=q: first(i, q).start())

    def first_wait(q):
        for i, (p, b, lo, skip, count) in enumerate(parts):
            if q in first_targets(b):
                @pl.when(jnp.logical_and(jnp.logical_and(c == 0, core == 0), plane == q))
                def _(i=i, b=b, skip=skip, count=count):
                    landing(wraw.at[b, pl.ds(skip, count)], w1_r.at[i])

    lead = core == 0

    def second(col):
        return remote(wraw.at[plane], wraw.at[plane], w2_s.at[col], w2_r, col=col)

    def second_all(act):
        for col in range(1, n_c):
            who = jnp.logical_and(lead, c == 0)
            if col == last:
                who = jnp.logical_and(who, plane == last)
            pl.when(who)(lambda col=col: act(second(col)))

    middle = jnp.logical_and(c > 0, c < last)
    spreads = jnp.logical_and(lead, jnp.logical_or(middle, jnp.logical_and(c == last, plane == last)))

    def third(k):
        to = lax.rem(plane + k, planes)
        return remote(
            wraw.at[plane], wraw.at[plane], w3_s.at[k], w3_r.at[plane], row=lax.div(to, n_d) * 2, depth=lax.rem(to, n_d)
        )

    def third_start():
        @pl.when(spreads)
        def _():
            landing(wraw.at[plane], w2_r)
            for k in range(1, planes):
                third(k).start()

    def fourth(whole):
        ref = wraw if whole else wraw.at[c]
        return remote(ref, ref, w4_s, w4_r, row=r + 1)

    def fourth_start():
        for q in range(n_c):
            other = plane != q
            need = middle if q != last else jnp.logical_or(middle, c == last)
            pl.when(jnp.logical_and(jnp.logical_and(lead, other), need))(lambda q=q: landing(wraw.at[q], w3_r.at[q]))
        pl.when(jnp.logical_and(lead, middle))(lambda: fourth(True).start())
        pl.when(jnp.logical_and(lead, jnp.logical_not(middle)))(lambda: fourth(False).start())

    def fourth_wait():
        pl.when(jnp.logical_and(core == 1, middle))(lambda: landing(wraw, w4_r))
        pl.when(jnp.logical_and(core == 1, jnp.logical_not(middle)))(lambda: landing(wraw.at[c], w4_r))

    load = pltpu.make_async_copy(panel, raw.at[0], own_s)
    load.start()
    keep = pltpu.make_async_copy(diag_ref, pieces.at[core, plane, c], piece_s)
    keep.start()
    fetch = pltpu.make_async_copy(trailing, trail, trail_s)
    fetch.start()
    for k in range(1, n_c):
        diag_z(k).start()
    load.wait()
    first_start()
    raw_start((0, 1), range(1))
    pl.when(c > 0)(lambda: raw_start((0, 1), range(1, split)))
    keep.wait()
    landing(pieces.at[core, plane, pl.ds(0, n_c - 1)], dz_r)
    for k in range(1, planes):
        diag_plane(k).start()
    raw_start((2,), range(split))
    landing(pieces.at[core, pl.ds(0, planes - 1)], dp_r)
    diag_core().start()
    landing(pieces.at[1 - core], dc_r)
    for p in range(total):
        p_r, p_c, p_d = p // (n_c * n_d), p // n_d % n_c, p % n_d
        mine = diag_ref.shape[0]
        work[p * mine : (p + 1) * mine, :] = pieces[p_r % 2, p_r // 2 * n_d + p_d, p_c]

    def second_start():
        for q in range(planes):
            first_wait(q)
        second_all(lambda copy: copy.start())
        pl.when(c == 0)(lambda: raw_start((0, 1), range(1, split)))

    stages = {1: second_start, 5: third_start, 7: fourth_start}

    def between(k, later):
        for point, action in stages.items():
            if point % 2 == later:
                pl.when(k == point // 2)(action)

    factor_all(work, low, inv, between)
    fourth_wait()

    dense[...] = dot(inv[...], inv[...], 0, 0)

    def make(q, carry):
        @pl.when(jnp.logical_or(middle, c == q))
        def _():
            mult[q] = dot(wraw[q], dense[...], 1, 0)

        return carry

    lax.fori_loop(0, n_c, make, 0)
    for h in range(split):
        for way in range(3):
            pl.when(comes[way])(lambda way=way, h=h: raw_copy(way, h).wait_recv())

    flip = c > last - c
    v_c = jnp.where(flip, last - c, c)
    v_d = jnp.where(flip, 1 - d, d)

    def task(k):
        edge = v_c == 0
        slot = jnp.where(edge, 2, jnp.where(k == 1, 2, jnp.where(k == 3, 2 - v_d, 1)))
        col = jnp.where(edge, 0, jnp.where(k == 0, 3, jnp.where(k == 1, 0, jnp.where(k == 2, 2, 1))))
        deep = jnp.where(edge, 0, jnp.where(k == 1, 1, jnp.where(k == 3, 1 - v_d, 0)))
        j = jnp.where(edge, 3, v_d)
        active = jnp.logical_or(v_c == 1, jnp.logical_and(v_d == 1, k == 0))
        return (
            active,
            jnp.where(flip, 3 - slot, slot),
            jnp.where(flip, last - col, col),
            jnp.where(flip, 1 - deep, deep),
            jnp.where(flip, 3 - j, j),
        )

    def prod_copy(t):
        k, h = lax.rem(t, 4), lax.div(t, 4)
        active, slot, col, deep, j = task(k)
        return active, remote(sent.at[k, at(h)], landed.at[j, at(h)], prod_s.at[k, h], prod_r.at[j, h], col=col, depth=deep)

    def launch(t):
        active, copy = prod_copy(t)
        pl.when(active)(lambda: copy.start())

    def produce(t, carry):
        k, h = lax.rem(t, 4), lax.div(t, 4)
        active, slot, col, deep, j = task(k)

        @pl.when(active)
        def _():
            sent[k, at(h), :] = dot(raw[slot, at(h), :], mult[col], 1, 1)

        pl.when(t > 0)(lambda: launch(t - 1))
        return carry

    lax.fori_loop(0, 4 * split, produce, 0)

    def local(j):
        cj, dj = d * per + lax.div(j, n_d), lax.rem(j, n_d)
        same = dj == d
        slot = jnp.where(cj == c, jnp.where(same, 0, 3), jnp.where(cj < c, 1, 2))
        close = jnp.logical_and(cj - c < 2, c - cj < 2)
        return jnp.logical_or(cj == c, jnp.logical_and(same, close)), slot

    def spot(t):
        return pl.ds(pl.multiple_of(t * size, 8), size)

    def out_copy(t):
        return pltpu.make_async_copy(trail.at[spot(t)], updated.at[spot(t)], out_s.at[t])

    def own_rows(h, carry):
        solved[at(h), :] = dot(raw[0, at(h), :], inv[...], 1, 1)
        return carry

    lax.fori_loop(0, split, own_rows, 0)
    launch(4 * split - 1)
    store = pltpu.make_async_copy(solved, solved_out, solved_s)
    fetch.wait()

    def consume(t, carry):
        j, h = lax.div(t, split), lax.rem(t, split)
        here, slot = local(j)

        @pl.when(here)
        def _():
            trail[spot(t), :] = trail[spot(t), :] - dot(raw[slot, at(h), :], mult[c], 1, 1)

        return carry

    lax.fori_loop(0, 4 * split, consume, 0)
    store.start()

    def flush(t, carry):
        here, slot = local(lax.div(t, split))
        pl.when(here)(lambda: out_copy(t).start())
        return carry

    lax.fori_loop(0, 4 * split, flush, 0)

    def receive(i, carry):
        h, j = lax.div(i, 4), lax.rem(i, 4)
        t = j * split + h
        here, slot = local(j)

        @pl.when(jnp.logical_not(here))
        def _():
            landing(landed.at[j, at(h)], prod_r.at[j, h])
            trail[spot(t), :] = trail[spot(t), :] - landed[j, at(h), :]
            out_copy(t).start()

        return carry

    lax.fori_loop(0, 4 * split, receive, 0)
    mine = diag_ref.shape[0]
    own[...] = low[pl.ds(pl.multiple_of(position * mine, 8), mine), :]

    for k in range(1, n_c):
        diag_z(k).wait_send()
    for k in range(1, planes):
        diag_plane(k).wait_send()
    diag_core().wait_send()
    for h in range(split):
        for way in range(3):
            pl.when(goes[way])(lambda way=way, h=h: raw_copy(way, h).wait_send())
    for i, (p, b, lo, skip, count) in enumerate(parts):
        for q in first_targets(b):
            if p != (q // n_d * 2 * n_c) * n_d + q % n_d:
                pl.when(position == p)(lambda i=i, q=q: first(i, q).wait_send())
    second_all(lambda copy: copy.wait_send())

    @pl.when(spreads)
    def _():
        for k in range(1, planes):
            third(k).wait_send()

    pl.when(jnp.logical_and(lead, middle))(lambda: fourth(True).wait_send())
    pl.when(jnp.logical_and(lead, jnp.logical_not(middle)))(lambda: fourth(False).wait_send())

    def drain(t, carry):
        active, copy = prod_copy(t)
        pl.when(active)(lambda: copy.wait_send())
        out_copy(t).wait()
        return carry

    lax.fori_loop(0, 4 * split, drain, 0)
    store.wait()


def near_call(sizes, diag_block, panel, trailing):
    n_r, n_c, n_d = sizes
    mine, n = diag_block.shape
    rows, width = panel.shape
    columns = trailing.shape[1]
    split = 2
    planes = n_r // 2 * n_d
    parts = []
    for p in range(-(-n_c * columns // rows)):
        for b in range(n_c):
            lo, hi = max(b * columns, p * rows), min((b + 1) * columns, (p + 1) * rows)
            if lo < hi:
                parts.append((p, b, lo - p * rows, lo - b * columns, hi - lo))
    vmem, anywhere = pl.BlockSpec(memory_space=pltpu.VMEM), pl.BlockSpec(memory_space=pl.ANY)
    dma = pltpu.SemaphoreType.DMA
    sems = [
        dma, dma, dma, dma((n_c,)), dma, dma((planes,)), dma, dma, dma, dma((3, split)), dma((3, split)),
        dma((len(parts), planes)), dma((len(parts),)), dma((n_c,)), dma, dma((planes,)), dma((planes,)), dma, dma,
        dma((4, split)), dma((4, split)), dma((4 * split,)), dma,
    ]
    square = pltpu.VMEM((n, n), jnp.float32)
    return pl.pallas_call(
        functools.partial(near, sizes, parts, split),
        out_shape=(
            jax.ShapeDtypeStruct((mine, n), jnp.float32),
            jax.ShapeDtypeStruct((rows, width), jnp.float32),
            jax.ShapeDtypeStruct(trailing.shape, jnp.float32),
        ),
        in_specs=[vmem, anywhere, anywhere],
        out_specs=(vmem, anywhere, anywhere),
        scratch_shapes=[
            pltpu.VMEM((4, rows, width), jnp.float32),
            pltpu.VMEM((n_c, columns, width), jnp.float32),
            pltpu.VMEM((n_c, columns, width), jnp.float32),
            pltpu.VMEM(trailing.shape, jnp.float32),
            pltpu.VMEM((rows, width), jnp.float32),
            pltpu.VMEM((4, rows, columns), jnp.float32),
            pltpu.VMEM((4, rows, columns), jnp.float32),
            pltpu.VMEM((2, planes, n_c, mine, n), jnp.float32),
            square, square, square, square,
            sems,
        ],
        compiler_params=pltpu.CompilerParams(has_side_effects=True, vmem_limit_bytes=63000000),
    )(diag_block, panel, trailing)


def body(sizes, diag_block, panel_rows, trailing):
    n_r, n_c, n_d = sizes
    if sizes == (4, 4, 2) and panel_rows.shape[0] % 16 == 0:
        return near_call(sizes, diag_block, panel_rows, trailing)
    position = (lax.axis_index("row") * n_c + lax.axis_index("col")) * n_d + lax.axis_index("depth")
    mine = diag_block.shape[0]
    own_rows, win_rows = trailing.shape
    rows, width = panel_rows.shape
    unit = math.gcd(rows, win_rows)
    low, weight, solved, held = exchange_call(
        sizes, diag_block, panel_rows.reshape(rows // unit, unit, width), win_rows // unit
    )
    own_factor = lax.dynamic_slice_in_dim(low, position * mine, mine, 0)
    updated = update_call(held.reshape(2 * n_c * rows, width), weight, trailing)
    return (own_factor, solved, updated)


def solution(mesh):
    sizes = tuple(mesh.shape[axis] for axis in AXES)
    specs = (P(AXES, None), P(AXES, None), P(("row", "depth"), "col"))
    return jax.shard_map(
        functools.partial(body, sizes), mesh=mesh, in_specs=specs, out_specs=specs, check_vma=False
    )
```

```python
import functools
import math

import jax
import jax.numpy as jnp
from jax import lax
from jax.experimental import pallas as pl
from jax.experimental.pallas import tpu as pltpu
from jax.sharding import PartitionSpec as P

highest = lax.Precision.HIGHEST
AXES = ("row", "col", "depth")
LANES = 128


def dot(left, right, left_dim, right_dim):
    return lax.dot_general(
        left, right, (((left_dim,), (right_dim,)), ((), ())), precision=highest, preferred_element_type=jnp.float32
    )


def factor_block(block, halfway=None):
    size = block.shape[0]
    step = 8
    lane = lax.broadcasted_iota(jnp.int32, (step, size), 1)
    sub = lax.broadcasted_iota(jnp.int32, (step, size), 0)
    tiles = [block[step * i : step * (i + 1), :] for i in range(size // step)]

    def across(tile, j):
        return jnp.broadcast_to(tile[:, j : j + 1], (step, size))

    def down(tile, s):
        return jnp.broadcast_to(tile[s : s + 1, :], (step, size))

    for t in range(size // step):
        if halfway is not None and t == size // step // 2:
            halfway()
        first = step * t
        tile = tiles[t]
        top = [across(tile, first + k) for k in range(step)]
        source, ratio = [], []
        for s in range(step):
            inverse = 1.0 / down(top[s], s)
            source.append(jnp.where(lane == first + s, 1.0, down(tile, s)) * inverse)
            ratio.append([down(top[k], s) * inverse for k in range(s + 1, step)])
            below = sub > s
            for k in range(s + 1, step):
                top[k] = jnp.where(below, top[k] - top[s] * ratio[s][k - s - 1], top[k])
            tile = jnp.where(below, jnp.where(lane == first + s, 0.0, tile) - top[s] * source[s], tile)
        if t + 1 < size // step:
            total = [jnp.where((lane > first + s) & (lane < first + step), 0.0, source[s]) for s in range(step)]
            for s in range(step - 2, -1, -1):
                for k in range(step - 1, s, -1):
                    total[s] = total[s] - ratio[s][k - s - 1] * total[k]
            panel = (lane >= first) & (lane < first + step)
            for i in range(t + 1, size // step):
                new = jnp.where(panel, 0.0, tiles[i])
                for s in range(step):
                    new = new - across(tiles[i], first + s) * total[s]
                tiles[i] = new
        tiles[t] = tile
    whole = jnp.concatenate(tiles, axis=0)
    r_id = lax.broadcasted_iota(jnp.int32, (size, size), 0)
    c_id = lax.broadcasted_iota(jnp.int32, (size, size), 1)
    pivots = jnp.sum(jnp.where(r_id == c_id, whole, 0.0), axis=1, keepdims=True)
    root = jnp.sqrt(pivots)
    scaled = jnp.where(r_id == c_id, 1.0, whole) / root
    inverse = jnp.where(r_id >= c_id, scaled, 0.0)
    upper = jnp.where(r_id < c_id, scaled, jnp.where(r_id == c_id, root, 0.0))
    return upper.T, inverse


def factor_all(work, low, inv, between=None):
    n = work.shape[0]
    low[...] = jnp.zeros((n, n), jnp.float32)
    inv[...] = jnp.zeros((n, n), jnp.float32)

    def step(k, carry):
        at = pl.ds(pl.multiple_of(k * LANES, LANES), LANES)
        halfway = None if between is None else functools.partial(between, k, 0)
        block_low, block_inv = factor_block(work[at, at], halfway)
        rows = lax.broadcasted_iota(jnp.int32, (n, LANES), 0)
        panel = jnp.where(rows >= (k + 1) * LANES, dot(work[:, at], block_inv, 1, 1), 0.0)
        work[...] = work[...] - dot(panel, panel, 1, 1)
        left = dot(low[at, :], inv[...], 1, 0)
        low[:, at] = panel
        low[at, at] = block_low
        inv[at, :] = -dot(block_inv, left, 1, 0)
        inv[at, at] = block_inv
        if between is not None:
            between(k, 1)
        return carry

    lax.fori_loop(0, n // LANES, step, 0)


def exchange(sizes, cuts, win_units, diag_ref, panel, low, weight, solved, held, window, pieces, work, inv, sems):
    n_r, n_c, n_d = sizes
    total = n_r * n_c * n_d
    half = n_c // 2
    units = panel.shape[0]
    (diag_s, diag_r, ring_s, ring_r, deep_s, deep_r, w1_s, w1_r, w2_s, w2_r, w3_s, w3_r, own_s) = sems
    r, c, d = lax.axis_index("row"), lax.axis_index("col"), lax.axis_index("depth")
    position = (r * n_c + c) * n_d + d

    def remote(src, dst, send, recv, **where):
        return pltpu.make_async_remote_copy(
            src_ref=src,
            dst_ref=dst,
            send_sem=send,
            recv_sem=recv,
            device_id={"row": where.get("row", r), "col": where.get("col", c), "depth": where.get("depth", d)},
            device_id_type=pl.DeviceIdType.MESH,
        )

    def taker(block):
        return lax.div(block * n_d + d, n_c)

    def slot(block):
        return jnp.where(taker(block) == d, block * n_d + d - n_c * d, n_c + block)

    def at(h):
        return pl.ds(cuts[h], cuts[h + 1] - cuts[h])

    def send_diag(k, carry):
        to = lax.rem(position + k, total)
        remote(
            diag_ref, pieces.at[position], diag_s, diag_r,
            row=lax.div(to, n_c * n_d), col=lax.rem(lax.div(to, n_d), n_c), depth=lax.rem(to, n_d),
        ).start()
        return carry

    lax.fori_loop(1, total, send_diag, 0)
    pieces[position] = diag_ref[...]

    def window_parts():
        for p in range(-(-n_c * win_units // units)):
            for b in range(n_c):
                lo, hi = max(b * win_units, p * units), min((b + 1) * win_units, (p + 1) * units)
                if lo < hi:
                    yield p, b, lo, hi - lo

    def part(p, b, lo, count):
        src = panel.at[pl.ds(lo - p * units, count)]
        dst = window.at[pl.ds(lo - b * win_units, count)]
        if p == b * n_d:
            return pltpu.make_async_copy(src, dst, w1_r.at[p])
        return remote(src, dst, w1_s.at[p, b], w1_r.at[p], row=0, col=b, depth=0)

    root = jnp.logical_and(r == 0, d == 0)
    for p, b, lo, count in window_parts():
        @pl.when(position == p)
        def _(p=p, b=b, lo=lo, count=count):
            part(p, b, lo, count).start()

    def to_depth(k):
        return remote(window, window, w2_s.at[k], w2_r, depth=k)

    def to_row(k):
        return remote(window, window, w3_s.at[k], w3_r, row=k)

    def window_second():
        for p, b, lo, count in window_parts():
            @pl.when(jnp.logical_and(root, c == b))
            def _(p=p, b=b, lo=lo, count=count):
                if p == b * n_d:
                    part(p, b, lo, count).wait()
                else:
                    piece = window.at[pl.ds(lo - b * win_units, count)]
                    pltpu.make_async_copy(piece, piece, w1_r.at[p]).wait()

        @pl.when(root)
        def _():
            for k in range(1, n_d):
                to_depth(k).start()

    def window_third():
        @pl.when(jnp.logical_and(r == 0, d != 0))
        def _():
            pltpu.make_async_copy(window, window, w2_r).wait()

        @pl.when(r == 0)
        def _():
            for k in range(1, n_r):
                to_row(k).start()

    def ring(way, s, h):
        block = lax.rem(c + n_c - s + 1, n_c) if way == 0 else lax.rem(c + s - 1, n_c)
        to = lax.rem(c + 1, n_c) if way == 0 else lax.rem(c + n_c - 1, n_c)
        dst = held.at[slot(block), at(h)]
        src = panel.at[at(h)] if s == 1 else dst
        return remote(src, dst, ring_s.at[way, s - 1, h], ring_r.at[way, s - 1, h], col=to)

    def ring_parts(s):
        return [(0, 0), (1, 1)] + ([(0, 1), (1, 0)] if s < half else [])

    def deep(step, h):
        block = lax.rem(c + n_c - step, n_c)
        to = taker(block)
        index = block * n_d + d - n_c * to
        src = panel.at[at(h)] if step == 0 else held.at[slot(block), at(h)]
        where = step + half - 1
        return to, remote(
            src, held.at[index, at(h)], deep_s.at[where, h], deep_r.at[index, h], depth=to
        )

    def start_deep(step, h):
        to, copy = deep(step, h)

        @pl.when(to != d)
        def _():
            copy.start()

    def own_copy():
        return pltpu.make_async_copy(panel, held.at[slot(c)], own_s)

    for way, h in ring_parts(1):
        ring(way, 1, h).start()
    for h in range(2):
        start_deep(0, h)

    @pl.when(taker(c) == d)
    def _():
        own_copy().start()

    def arrived(s, parts):
        for way, h in parts:
            ring(way, s, h).wait_recv()
            if s < half and (s + 1 < half or way == h):
                ring(way, s + 1, h).start()
            step = s if (way == 0 or s == half) else -s
            start_deep(step, h)

    def between(k, later):
        def when(point, action):
            if point % 2 == later:
                pl.when(k == point // 2)(action)

        when(1, window_second)
        when(3, window_third)
        if half > 1:
            when(2, lambda: arrived(1, ring_parts(1)[:2]))
            when(6, lambda: arrived(1, ring_parts(1)[2:]))

    every = pieces.at[pl.ds(0, total - 1)]
    pltpu.make_async_copy(every, every, diag_r).wait()
    mine = diag_ref.shape[0]
    for p in range(total):
        work[p * mine : (p + 1) * mine, :] = pieces[p]
    factor_all(work, low, inv, between)

    @pl.when(r != 0)
    def _():
        pltpu.make_async_copy(window, window, w3_r).wait()

    weight[...] = dot(dot(window[...].reshape(weight.shape), inv[...], 1, 1), inv[...], 1, 0)
    solved[...] = dot(panel[...].reshape(solved.shape), inv[...], 1, 1)
    for s in range(2 if half > 1 else 1, half + 1):
        arrived(s, ring_parts(s))

    for j in range(n_c):
        q = n_c * d + j

        @pl.when(lax.rem(q, n_d) != d)
        def _(j=j):
            for h in range(2):
                landed = held.at[j, at(h)]
                pltpu.make_async_copy(landed, landed, deep_r.at[j, h]).wait()

    pltpu.make_async_copy(every, every, diag_s).wait()
    for s in range(1, half + 1):
        for way, h in ring_parts(s):
            ring(way, s, h).wait_send()
    for step in range(1 - half, half + 1):
        for h in range(2):
            to, copy = deep(step, h)

            @pl.when(to != d)
            def _(copy=copy):
                copy.wait_send()

    @pl.when(taker(c) == d)
    def _():
        own_copy().wait()

    for p, b, lo, count in window_parts():
        if p != b * n_d:
            @pl.when(position == p)
            def _(p=p, b=b, lo=lo, count=count):
                part(p, b, lo, count).wait_send()

    @pl.when(root)
    def _():
        for k in range(1, n_d):
            to_depth(k).wait_send()

    @pl.when(r == 0)
    def _():
        for k in range(1, n_r):
            to_row(k).wait_send()


def exchange_call(sizes, diag_block, panel, win_units):
    n_r, n_c, n_d = sizes
    total = n_r * n_c * n_d
    units, unit, width = panel.shape
    n = diag_block.shape[1]
    square = jax.ShapeDtypeStruct((n, n), jnp.float32)
    vmem, anywhere = pl.BlockSpec(memory_space=pltpu.VMEM), pl.BlockSpec(memory_space=pl.ANY)
    dma, owners = pltpu.SemaphoreType.DMA, -(-n_c * win_units // units)
    sems = [
        dma, dma, dma((2, n_c // 2, 2)), dma((2, n_c // 2, 2)), dma((n_c, 2)), dma((n_c, 2)),
        dma((owners, n_c)), dma((owners,)), dma((n_d,)), dma, dma((n_r,)), dma, dma,
    ]
    return pl.pallas_call(
        functools.partial(exchange, sizes, (0, units // 2, units), win_units),
        out_shape=(
            square,
            jax.ShapeDtypeStruct((win_units * unit, width), jnp.float32),
            jax.ShapeDtypeStruct((units * unit, width), jnp.float32),
            jax.ShapeDtypeStruct((2 * n_c, units, unit, width), jnp.float32),
        ),
        in_specs=[vmem, vmem],
        out_specs=(vmem, vmem, vmem, anywhere),
        scratch_shapes=[
            pltpu.VMEM((win_units, unit, width), jnp.float32),
            pltpu.VMEM((total, diag_block.shape[0], n), jnp.float32),
            pltpu.VMEM((n, n), jnp.float32),
            pltpu.VMEM((n, n), jnp.float32),
            sems,
        ],
        compiler_params=pltpu.CompilerParams(has_side_effects=True),
    )(diag_block, panel)


def update(held, weight, trailing, out):
    out[...] = trailing[...] - dot(held[...], weight[...], 1, 1)


def update_call(held, weight, trailing):
    rows, columns = trailing.shape
    width = held.shape[1]
    chunk = max(m for m in range(8, 1025, 8) if rows % m == 0)
    return pl.pallas_call(
        update,
        grid=(rows // chunk,),
        out_shape=jax.ShapeDtypeStruct(trailing.shape, jnp.float32),
        in_specs=[
            pl.BlockSpec((chunk, width), lambda i: (i, 0)),
            pl.BlockSpec((columns, width), lambda i: (0, 0)),
            pl.BlockSpec((chunk, columns), lambda i: (i, 0)),
        ],
        out_specs=pl.BlockSpec((chunk, columns), lambda i: (i, 0)),
    )(held, weight, trailing)


def near(sizes, parts, split, diag_ref, panel, trailing, own, solved_out, updated, raw, wraw, mult, trail, solved, sent,
         landed, pieces, work, low, inv, dense, sems):
    n_r, n_c, n_d = sizes
    total = n_r * n_c * n_d
    planes = n_r // 2 * n_d
    last = n_c - 1
    per = n_c // n_d
    rows = raw.shape[1]
    size = rows // split
    part = wraw.shape[2]
    cuts = (0, size // 16 * 8, size, rows)
    raw_halves = [[(h, way) for h in range(3) for way in range(2) if (cuts[h] >= size) == bool(late)] for late in range(2)]
    order = sorted(range(len(parts)), key=lambda i: (-parts[i][1], parts[i][2]))
    (own_s, trail_s, piece_s, dz_s, dz_r, dp_s, dp_r, dc_s, dc_r, raw_s, raw_r, w1_s, w1_r, w2_s, w2_r, w3_s, w3_r, w4_s, w4_r,
     prod_s, prod_r, out_s, solved_s) = sems
    r, c, d = lax.axis_index("row"), lax.axis_index("col"), lax.axis_index("depth")
    y, core = lax.div(r, 2), lax.rem(r, 2)
    plane = y * n_d + d
    position = (r * n_c + c) * n_d + d

    def remote(src, dst, send, recv, **where):
        return pltpu.make_async_remote_copy(
            src_ref=src,
            dst_ref=dst,
            send_sem=send,
            recv_sem=recv,
            device_id={"row": where.get("row", r), "col": where.get("col", c), "depth": where.get("depth", d)},
            device_id_type=pl.DeviceIdType.MESH,
        )

    def at(h):
        return pl.ds(pl.multiple_of(h * size, 8), size)

    def landing(ref, sem):
        pltpu.make_async_copy(ref, ref, sem).wait()

    def diag_z(k):
        return remote(diag_ref, pieces.at[core, plane, c], dz_s.at[k], dz_r, col=lax.rem(c + k, n_c))

    def diag_plane(k):
        to = lax.rem(plane + k, planes)
        mine = pieces.at[core, plane]
        return remote(mine, mine, dp_s.at[k], dp_r, row=lax.div(to, n_d) * 2 + core, depth=lax.rem(to, n_d))

    def diag_core():
        return remote(pieces.at[core], pieces.at[core], dc_s, dc_r, row=y * 2 + 1 - core)

    takes = lax.div(c, per)
    goes = (c < last, c > 0, takes != d)
    comes = (c > 0, c < last, takes == d)
    steps = ({"col": c + 1}, {"col": c - 1}, {"depth": 1 - d})

    def raw_copy(way, h):
        span = pl.ds(cuts[h], cuts[h + 1] - cuts[h])
        return remote(raw.at[0, span], raw.at[way + 1, span], raw_s.at[way, h], raw_r.at[way, h], **steps[way])

    def raw_start(ways, hs):
        for h in hs:
            for way in ways:
                pl.when(goes[way])(lambda way=way, h=h: raw_copy(way, h).start())

    def first(i):
        p, e, lo, skip, count = parts[i]
        q, k = e // 2, e % 2
        src, dst = raw.at[0, pl.ds(lo, count)], wraw.at[k, q, pl.ds(skip, count)]
        row, depth = q // n_d * 2 + k, q % n_d
        if p == row * n_c * n_d + depth:
            return False, pltpu.make_async_copy(src, dst, w1_r.at[i])
        return True, remote(src, dst, w1_s.at[i], w1_r.at[i], row=row, col=0, depth=depth)

    def first_start():
        for i in order:
            pl.when(position == parts[i][0])(lambda i=i: first(i)[1].start())

    def first_wait():
        for i, (p, e, lo, skip, count) in enumerate(parts):
            @pl.when(jnp.logical_and(c == 0, plane * 2 + core == e))
            def _(i=i, e=e, skip=skip, count=count):
                landing(wraw.at[e % 2, e // 2, pl.ds(skip, count)], w1_r.at[i])

    middle = jnp.logical_and(c > 0, c < last)
    edge = jnp.logical_not(middle)
    mine_w = wraw.at[core, plane]

    def second(col):
        return remote(mine_w, mine_w, w2_s.at[col], w2_r, col=col)

    def second_all(act):
        for col in [*range(last - 1, 0, -1), last]:
            who = c == 0 if col < last else jnp.logical_and(c == 0, plane == last)
            pl.when(who)(lambda col=col: act(second(col)))

    spreads = jnp.logical_or(middle, jnp.logical_and(plane == c, edge))

    def third(k):
        to = lax.rem(plane + k, planes)
        return remote(mine_w, mine_w, w3_s.at[k], w3_r.at[plane], row=lax.div(to, n_d) * 2 + core, depth=lax.rem(to, n_d))

    def third_start():
        pl.when(jnp.logical_and(spreads, c > 0))(lambda: landing(mine_w, w2_r))

        @pl.when(spreads)
        def _():
            for k in range(1, planes):
                third(k).start()

        raw_start((2,), range(1, len(cuts) - 1))

    def fourth(whole):
        ref = wraw.at[core] if whole else wraw.at[core, c]
        return remote(ref, ref, w4_s, w4_r, row=y * 2 + 1 - core)

    def fourth_start():
        for q in range(n_c):
            need = jnp.logical_and(plane != q, jnp.logical_or(middle, c == q))
            pl.when(need)(lambda q=q: landing(wraw.at[core, q], w3_r.at[q]))
        pl.when(middle)(lambda: fourth(True).start())
        pl.when(edge)(lambda: fourth(False).start())

    def fourth_wait():
        pl.when(middle)(lambda: landing(wraw.at[1 - core], w4_r))
        pl.when(edge)(lambda: landing(wraw.at[1 - core, c], w4_r))

    load = pltpu.make_async_copy(panel, raw.at[0], own_s)
    load.start()
    keep = pltpu.make_async_copy(diag_ref, pieces.at[core, plane, c], piece_s)
    keep.start()
    fetch = pltpu.make_async_copy(trailing, trail, trail_s)
    fetch.start()
    for k in range(1, n_c):
        diag_z(k).start()
    load.wait()
    first_start()
    keep.wait()
    landing(pieces.at[core, plane, pl.ds(0, n_c - 1)], dz_r)
    for k in range(1, planes):
        diag_plane(k).start()
    raw_start((0, 1), range(1))
    pl.when(c > 0)(lambda: raw_start((0, 1), range(1, len(cuts) - 1)))
    first_wait()
    second_all(lambda copy: copy.start())
    pl.when(c == 0)(lambda: raw_start((0, 1), range(1, len(cuts) - 1)))
    raw_start((2,), range(1))
    landing(pieces.at[core, pl.ds(0, planes - 1)], dp_r)
    diag_core().start()
    landing(pieces.at[1 - core], dc_r)
    mine = diag_ref.shape[0]
    for p in range(total):
        p_r, p_c, p_d = p // (n_c * n_d), p // n_d % n_c, p % n_d
        work[p * mine : (p + 1) * mine, :] = pieces[p_r % 2, p_r // 2 * n_d + p_d, p_c]

    stages = {4: third_start, 7: fourth_start}

    def between(k, later):
        for point, action in stages.items():
            if point % 2 == later:
                pl.when(k == point // 2)(action)

    factor_all(work, low, inv, between)
    fourth_wait()

    flip = c > last - c
    v_c = jnp.where(flip, last - c, c)
    v_d = jnp.where(flip, 1 - d, d)

    def task(k):
        end = v_c == 0
        slot = jnp.where(end, 2, jnp.where(k == 1, 2, jnp.where(k == 3, 2 - v_d, 1)))
        col = jnp.where(end, 0, jnp.where(k == 0, 3, jnp.where(k == 1, 0, jnp.where(k == 2, 2, 1))))
        deep = jnp.where(end, 0, jnp.where(k == 1, 1, jnp.where(k == 3, 1 - v_d, 0)))
        j = jnp.where(end, 3, v_d)
        active = jnp.logical_or(v_c == 1, jnp.logical_and(v_d == 1, k == 0))
        return (
            active,
            jnp.where(flip, 3 - slot, slot),
            jnp.where(flip, last - col, col),
            jnp.where(flip, 1 - deep, deep),
            jnp.where(flip, 3 - j, j),
        )

    def prod_copy(t):
        k, h = lax.rem(t, 4), lax.div(t, 4)
        active, slot, col, deep, j = task(k)
        return active, remote(sent.at[k, at(h)], landed.at[j, at(h)], prod_s.at[k, h], prod_r.at[j, h], col=col, depth=deep)

    def launch(t):
        active, copy = prod_copy(t)
        pl.when(active)(lambda: copy.start())

    dense[...] = dot(inv[...], inv[...], 0, 0)
    for h, way in raw_halves[0]:
        pl.when(comes[way])(lambda way=way, h=h: raw_copy(way, h).wait_recv())

    def produce(t, carry):
        k, h = lax.rem(t, 4), lax.div(t, 4)
        active, slot, col, deep, j = task(k)

        @pl.when(jnp.logical_and(h == 0, jnp.logical_or(middle, k == 0)))
        def _():
            for i in range(2):
                mult[col, i * part : (i + 1) * part, :] = dot(wraw[i, col], dense[...], 1, 0)

        @pl.when(t == 4)
        def _():
            for h, way in raw_halves[1]:
                pl.when(comes[way])(lambda way=way, h=h: raw_copy(way, h).wait_recv())

        @pl.when(active)
        def _():
            sent[k, at(h), :] = dot(raw[slot, at(h), :], mult[col], 1, 1)

        pl.when(t > 0)(lambda: launch(t - 1))
        return carry

    lax.fori_loop(0, 4 * split, produce, 0)

    def local(j):
        cj, dj = d * per + lax.div(j, n_d), lax.rem(j, n_d)
        same = dj == d
        slot = jnp.where(cj == c, jnp.where(same, 0, 3), jnp.where(cj < c, 1, 2))
        close = jnp.logical_and(cj - c < 2, c - cj < 2)
        return jnp.logical_or(cj == c, jnp.logical_and(same, close)), slot

    def spot(t):
        return pl.ds(pl.multiple_of(t * size, 8), size)

    def out_copy(t):
        return pltpu.make_async_copy(trail.at[spot(t)], updated.at[spot(t)], out_s.at[t])

    def own_rows(h, carry):
        solved[at(h), :] = dot(raw[0, at(h), :], inv[...], 1, 1)
        return carry

    lax.fori_loop(0, split, own_rows, 0)
    launch(4 * split - 1)
    store = pltpu.make_async_copy(solved, solved_out, solved_s)
    fetch.wait()
    for h in range(len(cuts) - 1):
        pl.when(comes[2])(lambda h=h: raw_copy(2, h).wait_recv())

    def consume(t, carry):
        j, h = lax.div(t, split), lax.rem(t, split)
        here, slot = local(j)

        @pl.when(here)
        def _():
            trail[spot(t), :] = trail[spot(t), :] - dot(raw[slot, at(h), :], mult[c], 1, 1)

        return carry

    lax.fori_loop(0, 4 * split, consume, 0)
    store.start()

    def flush(t, carry):
        here, slot = local(lax.div(t, split))
        pl.when(here)(lambda: out_copy(t).start())
        return carry

    lax.fori_loop(0, 4 * split, flush, 0)

    def receive(i, carry):
        h, j = lax.div(i, 4), lax.rem(i, 4)
        t = j * split + h
        here, slot = local(j)

        @pl.when(jnp.logical_not(here))
        def _():
            landing(landed.at[j, at(h)], prod_r.at[j, h])
            trail[spot(t), :] = trail[spot(t), :] - landed[j, at(h), :]
            out_copy(t).start()

        return carry

    lax.fori_loop(0, 4 * split, receive, 0)
    own[...] = low[pl.ds(pl.multiple_of(position * mine, 8), mine), :]

    for k in range(1, n_c):
        diag_z(k).wait_send()
    for k in range(1, planes):
        diag_plane(k).wait_send()
    diag_core().wait_send()
    for h in range(len(cuts) - 1):
        for way in range(3):
            pl.when(goes[way])(lambda way=way, h=h: raw_copy(way, h).wait_send())
    for i in order:
        far, copy = first(i)
        if far:
            pl.when(position == parts[i][0])(lambda copy=copy: copy.wait_send())
    second_all(lambda copy: copy.wait_send())

    @pl.when(spreads)
    def _():
        for k in range(1, planes):
            third(k).wait_send()

    pl.when(middle)(lambda: fourth(True).wait_send())
    pl.when(edge)(lambda: fourth(False).wait_send())

    def drain(t, carry):
        active, copy = prod_copy(t)
        pl.when(active)(lambda: copy.wait_send())
        out_copy(t).wait()
        return carry

    lax.fori_loop(0, 4 * split, drain, 0)
    store.wait()


def near_call(sizes, diag_block, panel, trailing):
    n_r, n_c, n_d = sizes
    mine, n = diag_block.shape
    rows, width = panel.shape
    columns = trailing.shape[1]
    split = 2
    planes = n_r // 2 * n_d
    parts = []
    part = columns // 2
    for p in range(-(-n_c * columns // rows)):
        for e in range(2 * n_c):
            lo, hi = max(e * part, p * rows), min((e + 1) * part, (p + 1) * rows)
            if lo < hi:
                parts.append((p, e, lo - p * rows, lo - e * part, hi - lo))
    vmem, anywhere = pl.BlockSpec(memory_space=pltpu.VMEM), pl.BlockSpec(memory_space=pl.ANY)
    dma = pltpu.SemaphoreType.DMA
    sems = [
        dma, dma, dma, dma((n_c,)), dma, dma((planes,)), dma, dma, dma, dma((3, 3)), dma((3, 3)),
        dma((len(parts),)), dma((len(parts),)), dma((n_c,)), dma, dma((planes,)), dma((planes,)), dma, dma,
        dma((4, split)), dma((4, split)), dma((4 * split,)), dma,
    ]
    square = pltpu.VMEM((n, n), jnp.float32)
    return pl.pallas_call(
        functools.partial(near, sizes, parts, split),
        out_shape=(
            jax.ShapeDtypeStruct((mine, n), jnp.float32),
            jax.ShapeDtypeStruct((rows, width), jnp.float32),
            jax.ShapeDtypeStruct(trailing.shape, jnp.float32),
        ),
        in_specs=[vmem, anywhere, anywhere],
        out_specs=(vmem, anywhere, anywhere),
        scratch_shapes=[
            pltpu.VMEM((4, rows, width), jnp.float32),
            pltpu.VMEM((2, n_c, part, width), jnp.float32),
            pltpu.VMEM((n_c, columns, width), jnp.float32),
            pltpu.VMEM(trailing.shape, jnp.float32),
            pltpu.VMEM((rows, width), jnp.float32),
            pltpu.VMEM((4, rows, columns), jnp.float32),
            pltpu.VMEM((4, rows, columns), jnp.float32),
            pltpu.VMEM((2, planes, n_c, mine, n), jnp.float32),
            square, square, square, square,
            sems,
        ],
        compiler_params=pltpu.CompilerParams(has_side_effects=True, vmem_limit_bytes=63000000),
    )(diag_block, panel, trailing)


def body(sizes, diag_block, panel_rows, trailing):
    n_r, n_c, n_d = sizes
    if sizes == (4, 4, 2) and panel_rows.shape[0] % 16 == 0:
        return near_call(sizes, diag_block, panel_rows, trailing)
    position = (lax.axis_index("row") * n_c + lax.axis_index("col")) * n_d + lax.axis_index("depth")
    mine = diag_block.shape[0]
    own_rows, win_rows = trailing.shape
    rows, width = panel_rows.shape
    unit = math.gcd(rows, win_rows)
    low, weight, solved, held = exchange_call(
        sizes, diag_block, panel_rows.reshape(rows // unit, unit, width), win_rows // unit
    )
    own_factor = lax.dynamic_slice_in_dim(low, position * mine, mine, 0)
    updated = update_call(held.reshape(2 * n_c * rows, width), weight, trailing)
    return (own_factor, solved, updated)


def solution(mesh):
    sizes = tuple(mesh.shape[axis] for axis in AXES)
    specs = (P(AXES, None), P(AXES, None), P(("row", "depth"), "col"))
    return jax.shard_map(
        functools.partial(body, sizes), mesh=mesh, in_specs=specs, out_specs=specs, check_vma=False
    )
```

```python
import functools
import math

import jax
import jax.numpy as jnp
from jax import lax
from jax.experimental import pallas as pl
from jax.experimental.pallas import tpu as pltpu
from jax.sharding import PartitionSpec as P

highest = lax.Precision.HIGHEST
AXES = ("row", "col", "depth")
LANES = 128


def dot(left, right, left_dim, right_dim):
    return lax.dot_general(
        left, right, (((left_dim,), (right_dim,)), ((), ())), precision=highest, preferred_element_type=jnp.float32
    )


def factor_block(block, halfway=None):
    size = block.shape[0]
    step = 8
    lane = lax.broadcasted_iota(jnp.int32, (step, size), 1)
    sub = lax.broadcasted_iota(jnp.int32, (step, size), 0)
    tiles = [block[step * i : step * (i + 1), :] for i in range(size // step)]

    def across(tile, j):
        return jnp.broadcast_to(tile[:, j : j + 1], (step, size))

    def down(tile, s):
        return jnp.broadcast_to(tile[s : s + 1, :], (step, size))

    for t in range(size // step):
        if halfway is not None and t == size // step // 2:
            halfway()
        first = step * t
        tile = tiles[t]
        top = [across(tile, first + k) for k in range(step)]
        source, ratio = [], []
        for s in range(step):
            inverse = 1.0 / down(top[s], s)
            source.append(jnp.where(lane == first + s, 1.0, down(tile, s)) * inverse)
            ratio.append([down(top[k], s) * inverse for k in range(s + 1, step)])
            below = sub > s
            for k in range(s + 1, step):
                top[k] = jnp.where(below, top[k] - top[s] * ratio[s][k - s - 1], top[k])
            tile = jnp.where(below, jnp.where(lane == first + s, 0.0, tile) - top[s] * source[s], tile)
        if t + 1 < size // step:
            total = [jnp.where((lane > first + s) & (lane < first + step), 0.0, source[s]) for s in range(step)]
            for s in range(step - 2, -1, -1):
                for k in range(step - 1, s, -1):
                    total[s] = total[s] - ratio[s][k - s - 1] * total[k]
            panel = (lane >= first) & (lane < first + step)
            for i in range(t + 1, size // step):
                new = jnp.where(panel, 0.0, tiles[i])
                for s in range(step):
                    new = new - across(tiles[i], first + s) * total[s]
                tiles[i] = new
        tiles[t] = tile
    whole = jnp.concatenate(tiles, axis=0)
    r_id = lax.broadcasted_iota(jnp.int32, (size, size), 0)
    c_id = lax.broadcasted_iota(jnp.int32, (size, size), 1)
    pivots = jnp.sum(jnp.where(r_id == c_id, whole, 0.0), axis=1, keepdims=True)
    root = jnp.sqrt(pivots)
    scaled = jnp.where(r_id == c_id, 1.0, whole) / root
    inverse = jnp.where(r_id >= c_id, scaled, 0.0)
    upper = jnp.where(r_id < c_id, scaled, jnp.where(r_id == c_id, root, 0.0))
    return upper.T, inverse


def factor_all(work, low, inv, between=None):
    n = work.shape[0]
    low[...] = jnp.zeros((n, n), jnp.float32)
    inv[...] = jnp.zeros((n, n), jnp.float32)

    def step(k, carry):
        at = pl.ds(pl.multiple_of(k * LANES, LANES), LANES)
        halfway = None if between is None else functools.partial(between, k, 0)
        block_low, block_inv = factor_block(work[at, at], halfway)
        rows = lax.broadcasted_iota(jnp.int32, (n, LANES), 0)
        panel = jnp.where(rows >= (k + 1) * LANES, dot(work[:, at], block_inv, 1, 1), 0.0)
        work[...] = work[...] - dot(panel, panel, 1, 1)
        left = dot(low[at, :], inv[...], 1, 0)
        low[:, at] = panel
        low[at, at] = block_low
        inv[at, :] = -dot(block_inv, left, 1, 0)
        inv[at, at] = block_inv
        if between is not None:
            between(k, 1)
        return carry

    lax.fori_loop(0, n // LANES, step, 0)


def exchange(sizes, cuts, win_units, diag_ref, panel, low, weight, solved, held, window, pieces, work, inv, sems):
    n_r, n_c, n_d = sizes
    total = n_r * n_c * n_d
    half = n_c // 2
    units = panel.shape[0]
    (diag_s, diag_r, ring_s, ring_r, deep_s, deep_r, w1_s, w1_r, w2_s, w2_r, w3_s, w3_r, own_s) = sems
    r, c, d = lax.axis_index("row"), lax.axis_index("col"), lax.axis_index("depth")
    position = (r * n_c + c) * n_d + d

    def remote(src, dst, send, recv, **where):
        return pltpu.make_async_remote_copy(
            src_ref=src,
            dst_ref=dst,
            send_sem=send,
            recv_sem=recv,
            device_id={"row": where.get("row", r), "col": where.get("col", c), "depth": where.get("depth", d)},
            device_id_type=pl.DeviceIdType.MESH,
        )

    def taker(block):
        return lax.div(block * n_d + d, n_c)

    def slot(block):
        return jnp.where(taker(block) == d, block * n_d + d - n_c * d, n_c + block)

    def at(h):
        return pl.ds(cuts[h], cuts[h + 1] - cuts[h])

    def send_diag(k, carry):
        to = lax.rem(position + k, total)
        remote(
            diag_ref, pieces.at[position], diag_s, diag_r,
            row=lax.div(to, n_c * n_d), col=lax.rem(lax.div(to, n_d), n_c), depth=lax.rem(to, n_d),
        ).start()
        return carry

    lax.fori_loop(1, total, send_diag, 0)
    pieces[position] = diag_ref[...]

    def window_parts():
        for p in range(-(-n_c * win_units // units)):
            for b in range(n_c):
                lo, hi = max(b * win_units, p * units), min((b + 1) * win_units, (p + 1) * units)
                if lo < hi:
                    yield p, b, lo, hi - lo

    def part(p, b, lo, count):
        src = panel.at[pl.ds(lo - p * units, count)]
        dst = window.at[pl.ds(lo - b * win_units, count)]
        if p == b * n_d:
            return pltpu.make_async_copy(src, dst, w1_r.at[p])
        return remote(src, dst, w1_s.at[p, b], w1_r.at[p], row=0, col=b, depth=0)

    root = jnp.logical_and(r == 0, d == 0)
    for p, b, lo, count in window_parts():
        @pl.when(position == p)
        def _(p=p, b=b, lo=lo, count=count):
            part(p, b, lo, count).start()

    def to_depth(k):
        return remote(window, window, w2_s.at[k], w2_r, depth=k)

    def to_row(k):
        return remote(window, window, w3_s.at[k], w3_r, row=k)

    def window_second():
        for p, b, lo, count in window_parts():
            @pl.when(jnp.logical_and(root, c == b))
            def _(p=p, b=b, lo=lo, count=count):
                if p == b * n_d:
                    part(p, b, lo, count).wait()
                else:
                    piece = window.at[pl.ds(lo - b * win_units, count)]
                    pltpu.make_async_copy(piece, piece, w1_r.at[p]).wait()

        @pl.when(root)
        def _():
            for k in range(1, n_d):
                to_depth(k).start()

    def window_third():
        @pl.when(jnp.logical_and(r == 0, d != 0))
        def _():
            pltpu.make_async_copy(window, window, w2_r).wait()

        @pl.when(r == 0)
        def _():
            for k in range(1, n_r):
                to_row(k).start()

    def ring(way, s, h):
        block = lax.rem(c + n_c - s + 1, n_c) if way == 0 else lax.rem(c + s - 1, n_c)
        to = lax.rem(c + 1, n_c) if way == 0 else lax.rem(c + n_c - 1, n_c)
        dst = held.at[slot(block), at(h)]
        src = panel.at[at(h)] if s == 1 else dst
        return remote(src, dst, ring_s.at[way, s - 1, h], ring_r.at[way, s - 1, h], col=to)

    def ring_parts(s):
        return [(0, 0), (1, 1)] + ([(0, 1), (1, 0)] if s < half else [])

    def deep(step, h):
        block = lax.rem(c + n_c - step, n_c)
        to = taker(block)
        index = block * n_d + d - n_c * to
        src = panel.at[at(h)] if step == 0 else held.at[slot(block), at(h)]
        where = step + half - 1
        return to, remote(
            src, held.at[index, at(h)], deep_s.at[where, h], deep_r.at[index, h], depth=to
        )

    def start_deep(step, h):
        to, copy = deep(step, h)

        @pl.when(to != d)
        def _():
            copy.start()

    def own_copy():
        return pltpu.make_async_copy(panel, held.at[slot(c)], own_s)

    for way, h in ring_parts(1):
        ring(way, 1, h).start()
    for h in range(2):
        start_deep(0, h)

    @pl.when(taker(c) == d)
    def _():
        own_copy().start()

    def arrived(s, parts):
        for way, h in parts:
            ring(way, s, h).wait_recv()
            if s < half and (s + 1 < half or way == h):
                ring(way, s + 1, h).start()
            step = s if (way == 0 or s == half) else -s
            start_deep(step, h)

    def between(k, later):
        def when(point, action):
            if point % 2 == later:
                pl.when(k == point // 2)(action)

        when(1, window_second)
        when(3, window_third)
        if half > 1:
            when(2, lambda: arrived(1, ring_parts(1)[:2]))
            when(6, lambda: arrived(1, ring_parts(1)[2:]))

    every = pieces.at[pl.ds(0, total - 1)]
    pltpu.make_async_copy(every, every, diag_r).wait()
    mine = diag_ref.shape[0]
    for p in range(total):
        work[p * mine : (p + 1) * mine, :] = pieces[p]
    factor_all(work, low, inv, between)

    @pl.when(r != 0)
    def _():
        pltpu.make_async_copy(window, window, w3_r).wait()

    weight[...] = dot(dot(window[...].reshape(weight.shape), inv[...], 1, 1), inv[...], 1, 0)
    solved[...] = dot(panel[...].reshape(solved.shape), inv[...], 1, 1)
    for s in range(2 if half > 1 else 1, half + 1):
        arrived(s, ring_parts(s))

    for j in range(n_c):
        q = n_c * d + j

        @pl.when(lax.rem(q, n_d) != d)
        def _(j=j):
            for h in range(2):
                landed = held.at[j, at(h)]
                pltpu.make_async_copy(landed, landed, deep_r.at[j, h]).wait()

    pltpu.make_async_copy(every, every, diag_s).wait()
    for s in range(1, half + 1):
        for way, h in ring_parts(s):
            ring(way, s, h).wait_send()
    for step in range(1 - half, half + 1):
        for h in range(2):
            to, copy = deep(step, h)

            @pl.when(to != d)
            def _(copy=copy):
                copy.wait_send()

    @pl.when(taker(c) == d)
    def _():
        own_copy().wait()

    for p, b, lo, count in window_parts():
        if p != b * n_d:
            @pl.when(position == p)
            def _(p=p, b=b, lo=lo, count=count):
                part(p, b, lo, count).wait_send()

    @pl.when(root)
    def _():
        for k in range(1, n_d):
            to_depth(k).wait_send()

    @pl.when(r == 0)
    def _():
        for k in range(1, n_r):
            to_row(k).wait_send()


def exchange_call(sizes, diag_block, panel, win_units):
    n_r, n_c, n_d = sizes
    total = n_r * n_c * n_d
    units, unit, width = panel.shape
    n = diag_block.shape[1]
    square = jax.ShapeDtypeStruct((n, n), jnp.float32)
    vmem, anywhere = pl.BlockSpec(memory_space=pltpu.VMEM), pl.BlockSpec(memory_space=pl.ANY)
    dma, owners = pltpu.SemaphoreType.DMA, -(-n_c * win_units // units)
    sems = [
        dma, dma, dma((2, n_c // 2, 2)), dma((2, n_c // 2, 2)), dma((n_c, 2)), dma((n_c, 2)),
        dma((owners, n_c)), dma((owners,)), dma((n_d,)), dma, dma((n_r,)), dma, dma,
    ]
    return pl.pallas_call(
        functools.partial(exchange, sizes, (0, units // 2, units), win_units),
        out_shape=(
            square,
            jax.ShapeDtypeStruct((win_units * unit, width), jnp.float32),
            jax.ShapeDtypeStruct((units * unit, width), jnp.float32),
            jax.ShapeDtypeStruct((2 * n_c, units, unit, width), jnp.float32),
        ),
        in_specs=[vmem, vmem],
        out_specs=(vmem, vmem, vmem, anywhere),
        scratch_shapes=[
            pltpu.VMEM((win_units, unit, width), jnp.float32),
            pltpu.VMEM((total, diag_block.shape[0], n), jnp.float32),
            pltpu.VMEM((n, n), jnp.float32),
            pltpu.VMEM((n, n), jnp.float32),
            sems,
        ],
        compiler_params=pltpu.CompilerParams(has_side_effects=True),
    )(diag_block, panel)


def update(held, weight, trailing, out):
    out[...] = trailing[...] - dot(held[...], weight[...], 1, 1)


def update_call(held, weight, trailing):
    rows, columns = trailing.shape
    width = held.shape[1]
    chunk = max(m for m in range(8, 1025, 8) if rows % m == 0)
    return pl.pallas_call(
        update,
        grid=(rows // chunk,),
        out_shape=jax.ShapeDtypeStruct(trailing.shape, jnp.float32),
        in_specs=[
            pl.BlockSpec((chunk, width), lambda i: (i, 0)),
            pl.BlockSpec((columns, width), lambda i: (0, 0)),
            pl.BlockSpec((chunk, columns), lambda i: (i, 0)),
        ],
        out_specs=pl.BlockSpec((chunk, columns), lambda i: (i, 0)),
    )(held, weight, trailing)


def near(sizes, parts, split, diag_ref, panel, trailing, own, solved, trail, raw, wraw, mult, sent,
         landed, pieces, work, low, inv, dense, sems):
    n_r, n_c, n_d = sizes
    total = n_r * n_c * n_d
    planes = n_r // 2 * n_d
    last = n_c - 1
    per = n_c // n_d
    rows = raw.shape[1]
    size = rows // split
    part = wraw.shape[2]
    cuts = (0, size // 16 * 8, size, rows)
    raw_halves = [[(h, way) for h in range(3) for way in range(2) if (cuts[h] >= size) == bool(late)] for late in range(2)]
    order = sorted(range(len(parts)), key=lambda i: (-parts[i][1], parts[i][2]))
    (own_s, trail_s, piece_s, dz_s, dz_r, dp_s, dp_r, dc_s, dc_r, raw_s, raw_r, w1_s, w1_r, w2_s, w2_r, w3_s, w3_r, w4_s, w4_r,
     prod_s, prod_r) = sems
    r, c, d = lax.axis_index("row"), lax.axis_index("col"), lax.axis_index("depth")
    y, core = lax.div(r, 2), lax.rem(r, 2)
    plane = y * n_d + d
    position = (r * n_c + c) * n_d + d

    def remote(src, dst, send, recv, **where):
        return pltpu.make_async_remote_copy(
            src_ref=src,
            dst_ref=dst,
            send_sem=send,
            recv_sem=recv,
            device_id={"row": where.get("row", r), "col": where.get("col", c), "depth": where.get("depth", d)},
            device_id_type=pl.DeviceIdType.MESH,
        )

    def at(h):
        return pl.ds(pl.multiple_of(h * size, 8), size)

    def landing(ref, sem):
        pltpu.make_async_copy(ref, ref, sem).wait()

    def diag_z(k):
        return remote(pieces.at[core, plane, c], pieces.at[core, plane, c], dz_s.at[k], dz_r, col=lax.rem(c + k, n_c))

    def diag_plane(k):
        to = lax.rem(plane + k, planes)
        mine = pieces.at[core, plane]
        return remote(mine, mine, dp_s.at[k], dp_r, row=lax.div(to, n_d) * 2 + core, depth=lax.rem(to, n_d))

    def diag_core():
        return remote(pieces.at[core], pieces.at[core], dc_s, dc_r, row=y * 2 + 1 - core)

    takes = lax.div(c, per)
    goes = (c < last, c > 0, takes != d)
    comes = (c > 0, c < last, takes == d)
    steps = ({"col": c + 1}, {"col": c - 1}, {"depth": 1 - d})

    def raw_copy(way, h):
        span = pl.ds(cuts[h], cuts[h + 1] - cuts[h])
        return remote(raw.at[0, span], raw.at[way + 1, span], raw_s.at[way, h], raw_r.at[way, h], **steps[way])

    def raw_start(ways, hs):
        for h in hs:
            for way in ways:
                pl.when(goes[way])(lambda way=way, h=h: raw_copy(way, h).start())

    def first(i):
        p, e, lo, skip, count = parts[i]
        q, k = e // 2, e % 2
        src, dst = raw.at[0, pl.ds(lo, count)], wraw.at[k, q, pl.ds(skip, count)]
        row, depth = q // n_d * 2 + k, q % n_d
        if p == row * n_c * n_d + depth:
            return False, pltpu.make_async_copy(src, dst, w1_r.at[i])
        return True, remote(src, dst, w1_s.at[i], w1_r.at[i], row=row, col=0, depth=depth)

    def first_start():
        for i in order:
            pl.when(position == parts[i][0])(lambda i=i: first(i)[1].start())

    def first_wait():
        for i, (p, e, lo, skip, count) in enumerate(parts):
            @pl.when(jnp.logical_and(c == 0, plane * 2 + core == e))
            def _(i=i, e=e, skip=skip, count=count):
                landing(wraw.at[e % 2, e // 2, pl.ds(skip, count)], w1_r.at[i])

    middle = jnp.logical_and(c > 0, c < last)
    edge = jnp.logical_not(middle)
    mine_w = wraw.at[core, plane]

    def second(col):
        return remote(mine_w, mine_w, w2_s.at[col], w2_r, col=col)

    def second_all(act):
        for col in [*range(last - 1, 0, -1), last]:
            who = c == 0 if col < last else jnp.logical_and(c == 0, plane == last)
            pl.when(who)(lambda col=col: act(second(col)))

    spreads = jnp.logical_or(middle, jnp.logical_and(plane == c, edge))

    def third(k):
        to = lax.rem(plane + k, planes)
        return remote(mine_w, mine_w, w3_s.at[k], w3_r.at[plane], row=lax.div(to, n_d) * 2 + core, depth=lax.rem(to, n_d))

    def third_start():
        pl.when(jnp.logical_and(spreads, c > 0))(lambda: landing(mine_w, w2_r))

        @pl.when(spreads)
        def _():
            for k in range(1, planes):
                third(k).start()

        raw_start((2,), range(1, len(cuts) - 1))

    def fourth(whole):
        ref = wraw.at[core] if whole else wraw.at[core, c]
        return remote(ref, ref, w4_s, w4_r, row=y * 2 + 1 - core)

    def fourth_start():
        for q in range(n_c):
            need = jnp.logical_and(plane != q, jnp.logical_or(middle, c == q))
            pl.when(need)(lambda q=q: landing(wraw.at[core, q], w3_r.at[q]))
        pl.when(middle)(lambda: fourth(True).start())
        pl.when(edge)(lambda: fourth(False).start())

    def fourth_wait():
        pl.when(middle)(lambda: landing(wraw.at[1 - core], w4_r))
        pl.when(edge)(lambda: landing(wraw.at[1 - core, c], w4_r))

    keep = pltpu.make_async_copy(diag_ref, pieces.at[core, plane, c], piece_s)
    keep.start()
    load = pltpu.make_async_copy(panel, raw.at[0], own_s)
    load.start()
    fetch = pltpu.make_async_copy(trailing, trail, trail_s)
    fetch.start()
    gate = pltpu.get_barrier_semaphore()
    ring = n_c * n_d
    for k in range(1, ring):
        to = lax.rem(c * n_d + d + k, ring)
        pl.semaphore_signal(
            gate, inc=1, device_id={"row": r, "col": lax.div(to, n_d), "depth": lax.rem(to, n_d)},
            device_id_type=pl.DeviceIdType.MESH,
        )
    for k in range(1, n_r * n_d):
        to = lax.rem(r * n_d + d + k, n_r * n_d)
        far = lax.div(to, n_d) != r
        pl.when(far)(lambda to=to: pl.semaphore_signal(
            gate, inc=1, device_id={"row": lax.div(to, n_d), "col": c, "depth": lax.rem(to, n_d)},
            device_id_type=pl.DeviceIdType.MESH,
        ))
    pl.semaphore_wait(gate, ring - 1 + (n_r - 1) * n_d)
    keep.wait()
    for k in range(1, n_c):
        diag_z(k).start()
    load.wait()
    first_start()
    landing(pieces.at[core, plane, pl.ds(0, n_c - 1)], dz_r)
    for k in range(1, planes):
        diag_plane(k).start()
    raw_start((0, 1), range(1))
    pl.when(c > 0)(lambda: raw_start((0, 1), range(1, len(cuts) - 1)))
    first_wait()
    second_all(lambda copy: copy.start())
    pl.when(c == 0)(lambda: raw_start((0, 1), range(1, len(cuts) - 1)))
    raw_start((2,), range(1))
    landing(pieces.at[core, pl.ds(0, planes - 1)], dp_r)
    diag_core().start()
    landing(pieces.at[1 - core], dc_r)
    mine = diag_ref.shape[0]
    for p in range(total):
        p_r, p_c, p_d = p // (n_c * n_d), p // n_d % n_c, p % n_d
        work[p * mine : (p + 1) * mine, :] = pieces[p_r % 2, p_r // 2 * n_d + p_d, p_c]

    stages = {4: third_start, 7: fourth_start}

    def between(k, later):
        for point, action in stages.items():
            if point % 2 == later:
                pl.when(k == point // 2)(action)

    factor_all(work, low, inv, between)
    fourth_wait()

    flip = c > last - c
    v_c = jnp.where(flip, last - c, c)
    v_d = jnp.where(flip, 1 - d, d)

    def task(k):
        end = v_c == 0
        slot = jnp.where(end, 2, jnp.where(k == 1, 2, jnp.where(k == 3, 2 - v_d, 1)))
        col = jnp.where(end, 0, jnp.where(k == 0, 3, jnp.where(k == 1, 0, jnp.where(k == 2, 2, 1))))
        deep = jnp.where(end, 0, jnp.where(k == 1, 1, jnp.where(k == 3, 1 - v_d, 0)))
        j = jnp.where(end, 3, v_d)
        active = jnp.logical_or(v_c == 1, jnp.logical_and(v_d == 1, k == 0))
        return (
            active,
            jnp.where(flip, 3 - slot, slot),
            jnp.where(flip, last - col, col),
            jnp.where(flip, 1 - deep, deep),
            jnp.where(flip, 3 - j, j),
        )

    def prod_copy(t):
        k, h = lax.rem(t, 4), lax.div(t, 4)
        active, slot, col, deep, j = task(k)
        return active, remote(sent.at[k, at(h)], landed.at[j, at(h)], prod_s.at[k, h], prod_r.at[j, h], col=col, depth=deep)

    def launch(t):
        active, copy = prod_copy(t)
        pl.when(active)(lambda: copy.start())

    dense[...] = dot(inv[...], inv[...], 0, 0)
    for h, way in raw_halves[0]:
        pl.when(comes[way])(lambda way=way, h=h: raw_copy(way, h).wait_recv())

    def produce(t, carry):
        k, h = lax.rem(t, 4), lax.div(t, 4)
        active, slot, col, deep, j = task(k)

        @pl.when(jnp.logical_and(h == 0, jnp.logical_or(middle, k == 0)))
        def _():
            for i in range(2):
                mult[col, i * part : (i + 1) * part, :] = dot(wraw[i, col], dense[...], 1, 0)

        @pl.when(t == 4)
        def _():
            for h, way in raw_halves[1]:
                pl.when(comes[way])(lambda way=way, h=h: raw_copy(way, h).wait_recv())

        @pl.when(active)
        def _():
            sent[k, at(h), :] = dot(raw[slot, at(h), :], mult[col], 1, 1)

        pl.when(t > 0)(lambda: launch(t - 1))
        return carry

    lax.fori_loop(0, 4 * split, produce, 0)

    def local(j):
        cj, dj = d * per + lax.div(j, n_d), lax.rem(j, n_d)
        same = dj == d
        slot = jnp.where(cj == c, jnp.where(same, 0, 3), jnp.where(cj < c, 1, 2))
        close = jnp.logical_and(cj - c < 2, c - cj < 2)
        return jnp.logical_or(cj == c, jnp.logical_and(same, close)), slot

    def spot(t):
        return pl.ds(pl.multiple_of(t * size, 8), size)

    def own_rows(h, carry):
        solved[at(h), :] = dot(raw[0, at(h), :], inv[...], 1, 1)
        return carry

    lax.fori_loop(0, split, own_rows, 0)
    launch(4 * split - 1)
    fetch.wait()
    for h in range(len(cuts) - 1):
        pl.when(comes[2])(lambda h=h: raw_copy(2, h).wait_recv())

    def consume(t, carry):
        j, h = lax.div(t, split), lax.rem(t, split)
        here, slot = local(j)

        @pl.when(here)
        def _():
            trail[spot(t), :] = trail[spot(t), :] - dot(raw[slot, at(h), :], mult[c], 1, 1)

        return carry

    lax.fori_loop(0, 4 * split, consume, 0)

    def receive(i, carry):
        h, j = lax.div(i, 4), lax.rem(i, 4)
        t = j * split + h
        here, slot = local(j)

        @pl.when(jnp.logical_not(here))
        def _():
            landing(landed.at[j, at(h)], prod_r.at[j, h])
            trail[spot(t), :] = trail[spot(t), :] - landed[j, at(h), :]

        return carry

    lax.fori_loop(0, 4 * split, receive, 0)
    own[...] = low[pl.ds(pl.multiple_of(position * mine, 8), mine), :]

    for k in range(1, n_c):
        diag_z(k).wait_send()
    for k in range(1, planes):
        diag_plane(k).wait_send()
    diag_core().wait_send()
    for h in range(len(cuts) - 1):
        for way in range(3):
            pl.when(goes[way])(lambda way=way, h=h: raw_copy(way, h).wait_send())
    for i in order:
        far, copy = first(i)
        if far:
            pl.when(position == parts[i][0])(lambda copy=copy: copy.wait_send())
    second_all(lambda copy: copy.wait_send())

    @pl.when(spreads)
    def _():
        for k in range(1, planes):
            third(k).wait_send()

    pl.when(middle)(lambda: fourth(True).wait_send())
    pl.when(edge)(lambda: fourth(False).wait_send())

    def drain(t, carry):
        active, copy = prod_copy(t)
        pl.when(active)(lambda: copy.wait_send())
        return carry

    lax.fori_loop(0, 4 * split, drain, 0)


def near_call(sizes, diag_block, panel, trailing):
    n_r, n_c, n_d = sizes
    mine, n = diag_block.shape
    rows, width = panel.shape
    columns = trailing.shape[1]
    split = 2
    planes = n_r // 2 * n_d
    parts = []
    part = columns // 2
    for p in range(-(-n_c * columns // rows)):
        for e in range(2 * n_c):
            lo, hi = max(e * part, p * rows), min((e + 1) * part, (p + 1) * rows)
            if lo < hi:
                parts.append((p, e, lo - p * rows, lo - e * part, hi - lo))
    vmem, anywhere = pl.BlockSpec(memory_space=pltpu.VMEM), pl.BlockSpec(memory_space=pl.ANY)
    dma = pltpu.SemaphoreType.DMA
    sems = [
        dma, dma, dma, dma((n_c,)), dma, dma((planes,)), dma, dma, dma, dma((3, 3)), dma((3, 3)),
        dma((len(parts),)), dma((len(parts),)), dma((n_c,)), dma, dma((planes,)), dma((planes,)), dma, dma,
        dma((4, split)), dma((4, split)),
    ]
    square = pltpu.VMEM((n, n), jnp.float32)
    return pl.pallas_call(
        functools.partial(near, sizes, parts, split),
        out_shape=(
            jax.ShapeDtypeStruct((mine, n), jnp.float32),
            jax.ShapeDtypeStruct((rows, width), jnp.float32),
            jax.ShapeDtypeStruct(trailing.shape, jnp.float32),
        ),
        in_specs=[pl.BlockSpec(memory_space=pltpu.HBM)] * 3,
        out_specs=(vmem, vmem, vmem),
        scratch_shapes=[
            pltpu.VMEM((4, rows, width), jnp.float32),
            pltpu.VMEM((2, n_c, part, width), jnp.float32),
            pltpu.VMEM((n_c, columns, width), jnp.float32),
            pltpu.VMEM((4, rows, columns), jnp.float32),
            pltpu.VMEM((4, rows, columns), jnp.float32),
            pltpu.VMEM((2, planes, n_c, mine, n), jnp.float32),
            square, square, square, square,
            sems,
        ],
        compiler_params=pltpu.CompilerParams(collective_id=0, has_side_effects=True, vmem_limit_bytes=40000000),
    )(*(pltpu.with_memory_space_constraint(x, pltpu.HBM) for x in (diag_block, panel, trailing)))


def body(sizes, diag_block, panel_rows, trailing):
    n_r, n_c, n_d = sizes
    if sizes == (4, 4, 2) and panel_rows.shape[0] % 16 == 0:
        return near_call(sizes, diag_block, panel_rows, trailing)
    position = (lax.axis_index("row") * n_c + lax.axis_index("col")) * n_d + lax.axis_index("depth")
    mine = diag_block.shape[0]
    own_rows, win_rows = trailing.shape
    rows, width = panel_rows.shape
    unit = math.gcd(rows, win_rows)
    low, weight, solved, held = exchange_call(
        sizes, diag_block, panel_rows.reshape(rows // unit, unit, width), win_rows // unit
    )
    own_factor = lax.dynamic_slice_in_dim(low, position * mine, mine, 0)
    updated = update_call(held.reshape(2 * n_c * rows, width), weight, trailing)
    return (own_factor, solved, updated)


def solution(mesh):
    sizes = tuple(mesh.shape[axis] for axis in AXES)
    specs = (P(AXES, None), P(AXES, None), P(("row", "depth"), "col"))
    return jax.shard_map(
        functools.partial(body, sizes), mesh=mesh, in_specs=specs, out_specs=specs, check_vma=False
    )
```

```python
import functools
import math

import jax
import jax.numpy as jnp
from jax import lax
from jax.experimental import pallas as pl
from jax.experimental.pallas import tpu as pltpu
from jax.sharding import PartitionSpec as P

highest = lax.Precision.HIGHEST
AXES = ("row", "col", "depth")
LANES = 128


def dot(left, right, left_dim, right_dim):
    return lax.dot_general(
        left, right, (((left_dim,), (right_dim,)), ((), ())), precision=highest, preferred_element_type=jnp.float32
    )


def factor_block(block, halfway=None):
    size = block.shape[0]
    step = 8
    lane = lax.broadcasted_iota(jnp.int32, (step, size), 1)
    sub = lax.broadcasted_iota(jnp.int32, (step, size), 0)
    tiles = [block[step * i : step * (i + 1), :] for i in range(size // step)]

    def across(tile, j):
        return jnp.broadcast_to(tile[:, j : j + 1], (step, size))

    def down(tile, s):
        return jnp.broadcast_to(tile[s : s + 1, :], (step, size))

    for t in range(size // step):
        if halfway is not None and t == size // step // 2:
            halfway()
        first = step * t
        tile = tiles[t]
        top = [across(tile, first + k) for k in range(step)]
        source, ratio = [], []
        for s in range(step):
            inverse = 1.0 / down(top[s], s)
            source.append(jnp.where(lane == first + s, 1.0, down(tile, s)) * inverse)
            ratio.append([down(top[k], s) * inverse for k in range(s + 1, step)])
            below = sub > s
            for k in range(s + 1, step):
                top[k] = jnp.where(below, top[k] - top[s] * ratio[s][k - s - 1], top[k])
            tile = jnp.where(below, jnp.where(lane == first + s, 0.0, tile) - top[s] * source[s], tile)
        if t + 1 < size // step:
            total = [jnp.where((lane > first + s) & (lane < first + step), 0.0, source[s]) for s in range(step)]
            for s in range(step - 2, -1, -1):
                for k in range(step - 1, s, -1):
                    total[s] = total[s] - ratio[s][k - s - 1] * total[k]
            panel = (lane >= first) & (lane < first + step)
            for i in range(t + 1, size // step):
                new = jnp.where(panel, 0.0, tiles[i])
                for s in range(step):
                    new = new - across(tiles[i], first + s) * total[s]
                tiles[i] = new
        tiles[t] = tile
    whole = jnp.concatenate(tiles, axis=0)
    r_id = lax.broadcasted_iota(jnp.int32, (size, size), 0)
    c_id = lax.broadcasted_iota(jnp.int32, (size, size), 1)
    pivots = jnp.sum(jnp.where(r_id == c_id, whole, 0.0), axis=1, keepdims=True)
    root = jnp.sqrt(pivots)
    scaled = jnp.where(r_id == c_id, 1.0, whole) / root
    inverse = jnp.where(r_id >= c_id, scaled, 0.0)
    upper = jnp.where(r_id < c_id, scaled, jnp.where(r_id == c_id, root, 0.0))
    return upper.T, inverse


def factor_all(work, low, inv, between=None):
    n = work.shape[0]
    low[...] = jnp.zeros((n, n), jnp.float32)
    inv[...] = jnp.zeros((n, n), jnp.float32)

    def step(k, carry):
        at = pl.ds(pl.multiple_of(k * LANES, LANES), LANES)
        halfway = None if between is None else functools.partial(between, k, 0)
        block_low, block_inv = factor_block(work[at, at], halfway)
        rows = lax.broadcasted_iota(jnp.int32, (n, LANES), 0)
        panel = jnp.where(rows >= (k + 1) * LANES, dot(work[:, at], block_inv, 1, 1), 0.0)
        work[...] = work[...] - dot(panel, panel, 1, 1)
        left = dot(low[at, :], inv[...], 1, 0)
        low[:, at] = panel
        low[at, at] = block_low
        inv[at, :] = -dot(block_inv, left, 1, 0)
        inv[at, at] = block_inv
        if between is not None:
            between(k, 1)
        return carry

    lax.fori_loop(0, n // LANES, step, 0)


def exchange(sizes, cuts, win_units, diag_ref, panel, low, weight, solved, held, window, pieces, work, inv, sems):
    n_r, n_c, n_d = sizes
    total = n_r * n_c * n_d
    half = n_c // 2
    units = panel.shape[0]
    (diag_s, diag_r, ring_s, ring_r, deep_s, deep_r, w1_s, w1_r, w2_s, w2_r, w3_s, w3_r, own_s) = sems
    r, c, d = lax.axis_index("row"), lax.axis_index("col"), lax.axis_index("depth")
    position = (r * n_c + c) * n_d + d

    def remote(src, dst, send, recv, **where):
        return pltpu.make_async_remote_copy(
            src_ref=src,
            dst_ref=dst,
            send_sem=send,
            recv_sem=recv,
            device_id={"row": where.get("row", r), "col": where.get("col", c), "depth": where.get("depth", d)},
            device_id_type=pl.DeviceIdType.MESH,
        )

    def taker(block):
        return lax.div(block * n_d + d, n_c)

    def slot(block):
        return jnp.where(taker(block) == d, block * n_d + d - n_c * d, n_c + block)

    def at(h):
        return pl.ds(cuts[h], cuts[h + 1] - cuts[h])

    def send_diag(k, carry):
        to = lax.rem(position + k, total)
        remote(
            diag_ref, pieces.at[position], diag_s, diag_r,
            row=lax.div(to, n_c * n_d), col=lax.rem(lax.div(to, n_d), n_c), depth=lax.rem(to, n_d),
        ).start()
        return carry

    lax.fori_loop(1, total, send_diag, 0)
    pieces[position] = diag_ref[...]

    def window_parts():
        for p in range(-(-n_c * win_units // units)):
            for b in range(n_c):
                lo, hi = max(b * win_units, p * units), min((b + 1) * win_units, (p + 1) * units)
                if lo < hi:
                    yield p, b, lo, hi - lo

    def part(p, b, lo, count):
        src = panel.at[pl.ds(lo - p * units, count)]
        dst = window.at[pl.ds(lo - b * win_units, count)]
        if p == b * n_d:
            return pltpu.make_async_copy(src, dst, w1_r.at[p])
        return remote(src, dst, w1_s.at[p, b], w1_r.at[p], row=0, col=b, depth=0)

    root = jnp.logical_and(r == 0, d == 0)
    for p, b, lo, count in window_parts():
        @pl.when(position == p)
        def _(p=p, b=b, lo=lo, count=count):
            part(p, b, lo, count).start()

    def to_depth(k):
        return remote(window, window, w2_s.at[k], w2_r, depth=k)

    def to_row(k):
        return remote(window, window, w3_s.at[k], w3_r, row=k)

    def window_second():
        for p, b, lo, count in window_parts():
            @pl.when(jnp.logical_and(root, c == b))
            def _(p=p, b=b, lo=lo, count=count):
                if p == b * n_d:
                    part(p, b, lo, count).wait()
                else:
                    piece = window.at[pl.ds(lo - b * win_units, count)]
                    pltpu.make_async_copy(piece, piece, w1_r.at[p]).wait()

        @pl.when(root)
        def _():
            for k in range(1, n_d):
                to_depth(k).start()

    def window_third():
        @pl.when(jnp.logical_and(r == 0, d != 0))
        def _():
            pltpu.make_async_copy(window, window, w2_r).wait()

        @pl.when(r == 0)
        def _():
            for k in range(1, n_r):
                to_row(k).start()

    def ring(way, s, h):
        block = lax.rem(c + n_c - s + 1, n_c) if way == 0 else lax.rem(c + s - 1, n_c)
        to = lax.rem(c + 1, n_c) if way == 0 else lax.rem(c + n_c - 1, n_c)
        dst = held.at[slot(block), at(h)]
        src = panel.at[at(h)] if s == 1 else dst
        return remote(src, dst, ring_s.at[way, s - 1, h], ring_r.at[way, s - 1, h], col=to)

    def ring_parts(s):
        return [(0, 0), (1, 1)] + ([(0, 1), (1, 0)] if s < half else [])

    def deep(step, h):
        block = lax.rem(c + n_c - step, n_c)
        to = taker(block)
        index = block * n_d + d - n_c * to
        src = panel.at[at(h)] if step == 0 else held.at[slot(block), at(h)]
        where = step + half - 1
        return to, remote(
            src, held.at[index, at(h)], deep_s.at[where, h], deep_r.at[index, h], depth=to
        )

    def start_deep(step, h):
        to, copy = deep(step, h)

        @pl.when(to != d)
        def _():
            copy.start()

    def own_copy():
        return pltpu.make_async_copy(panel, held.at[slot(c)], own_s)

    for way, h in ring_parts(1):
        ring(way, 1, h).start()
    for h in range(2):
        start_deep(0, h)

    @pl.when(taker(c) == d)
    def _():
        own_copy().start()

    def arrived(s, parts):
        for way, h in parts:
            ring(way, s, h).wait_recv()
            if s < half and (s + 1 < half or way == h):
                ring(way, s + 1, h).start()
            step = s if (way == 0 or s == half) else -s
            start_deep(step, h)

    def between(k, later):
        def when(point, action):
            if point % 2 == later:
                pl.when(k == point // 2)(action)

        when(1, window_second)
        when(3, window_third)
        if half > 1:
            when(2, lambda: arrived(1, ring_parts(1)[:2]))
            when(6, lambda: arrived(1, ring_parts(1)[2:]))

    every = pieces.at[pl.ds(0, total - 1)]
    pltpu.make_async_copy(every, every, diag_r).wait()
    mine = diag_ref.shape[0]
    for p in range(total):
        work[p * mine : (p + 1) * mine, :] = pieces[p]
    factor_all(work, low, inv, between)

    @pl.when(r != 0)
    def _():
        pltpu.make_async_copy(window, window, w3_r).wait()

    weight[...] = dot(dot(window[...].reshape(weight.shape), inv[...], 1, 1), inv[...], 1, 0)
    solved[...] = dot(panel[...].reshape(solved.shape), inv[...], 1, 1)
    for s in range(2 if half > 1 else 1, half + 1):
        arrived(s, ring_parts(s))

    for j in range(n_c):
        q = n_c * d + j

        @pl.when(lax.rem(q, n_d) != d)
        def _(j=j):
            for h in range(2):
                landed = held.at[j, at(h)]
                pltpu.make_async_copy(landed, landed, deep_r.at[j, h]).wait()

    pltpu.make_async_copy(every, every, diag_s).wait()
    for s in range(1, half + 1):
        for way, h in ring_parts(s):
            ring(way, s, h).wait_send()
    for step in range(1 - half, half + 1):
        for h in range(2):
            to, copy = deep(step, h)

            @pl.when(to != d)
            def _(copy=copy):
                copy.wait_send()

    @pl.when(taker(c) == d)
    def _():
        own_copy().wait()

    for p, b, lo, count in window_parts():
        if p != b * n_d:
            @pl.when(position == p)
            def _(p=p, b=b, lo=lo, count=count):
                part(p, b, lo, count).wait_send()

    @pl.when(root)
    def _():
        for k in range(1, n_d):
            to_depth(k).wait_send()

    @pl.when(r == 0)
    def _():
        for k in range(1, n_r):
            to_row(k).wait_send()


def exchange_call(sizes, diag_block, panel, win_units):
    n_r, n_c, n_d = sizes
    total = n_r * n_c * n_d
    units, unit, width = panel.shape
    n = diag_block.shape[1]
    square = jax.ShapeDtypeStruct((n, n), jnp.float32)
    vmem, anywhere = pl.BlockSpec(memory_space=pltpu.VMEM), pl.BlockSpec(memory_space=pl.ANY)
    dma, owners = pltpu.SemaphoreType.DMA, -(-n_c * win_units // units)
    sems = [
        dma, dma, dma((2, n_c // 2, 2)), dma((2, n_c // 2, 2)), dma((n_c, 2)), dma((n_c, 2)),
        dma((owners, n_c)), dma((owners,)), dma((n_d,)), dma, dma((n_r,)), dma, dma,
    ]
    return pl.pallas_call(
        functools.partial(exchange, sizes, (0, units // 2, units), win_units),
        out_shape=(
            square,
            jax.ShapeDtypeStruct((win_units * unit, width), jnp.float32),
            jax.ShapeDtypeStruct((units * unit, width), jnp.float32),
            jax.ShapeDtypeStruct((2 * n_c, units, unit, width), jnp.float32),
        ),
        in_specs=[vmem, vmem],
        out_specs=(vmem, vmem, vmem, anywhere),
        scratch_shapes=[
            pltpu.VMEM((win_units, unit, width), jnp.float32),
            pltpu.VMEM((total, diag_block.shape[0], n), jnp.float32),
            pltpu.VMEM((n, n), jnp.float32),
            pltpu.VMEM((n, n), jnp.float32),
            sems,
        ],
        compiler_params=pltpu.CompilerParams(has_side_effects=True),
    )(diag_block, panel)


def update(held, weight, trailing, out):
    out[...] = trailing[...] - dot(held[...], weight[...], 1, 1)


def update_call(held, weight, trailing):
    rows, columns = trailing.shape
    width = held.shape[1]
    chunk = max(m for m in range(8, 1025, 8) if rows % m == 0)
    return pl.pallas_call(
        update,
        grid=(rows // chunk,),
        out_shape=jax.ShapeDtypeStruct(trailing.shape, jnp.float32),
        in_specs=[
            pl.BlockSpec((chunk, width), lambda i: (i, 0)),
            pl.BlockSpec((columns, width), lambda i: (0, 0)),
            pl.BlockSpec((chunk, columns), lambda i: (i, 0)),
        ],
        out_specs=pl.BlockSpec((chunk, columns), lambda i: (i, 0)),
    )(held, weight, trailing)


def near(sizes, parts, split, diag_ref, panel, trailing, own, solved, trail, raw, wraw, mult, sent,
         landed, pieces, work, low, inv, dense, sems):
    n_r, n_c, n_d = sizes
    total = n_r * n_c * n_d
    planes = n_r // 2 * n_d
    last = n_c - 1
    per = n_c // n_d
    rows = raw.shape[1]
    size = rows // split
    cuts = (0, size // 16 * 8, size, rows)
    raw_halves = [[(h, way) for h in range(3) for way in range(2) if (cuts[h] >= size) == bool(late)] for late in range(2)]
    (own_s, trail_s, piece_s, dz_s, dz_r, dp_s, dp_r, dc_s, dc_r, raw_s, raw_r, w1_s, w1_r, w2_s, w2_r, w3_s, w3_r, w4_s, w4_r,
     prod_s, prod_r) = sems
    r, c, d = lax.axis_index("row"), lax.axis_index("col"), lax.axis_index("depth")
    y, core = lax.div(r, 2), lax.rem(r, 2)
    plane = y * n_d + d
    position = (r * n_c + c) * n_d + d

    def remote(src, dst, send, recv, **where):
        return pltpu.make_async_remote_copy(
            src_ref=src,
            dst_ref=dst,
            send_sem=send,
            recv_sem=recv,
            device_id={"row": where.get("row", r), "col": where.get("col", c), "depth": where.get("depth", d)},
            device_id_type=pl.DeviceIdType.MESH,
        )

    def at(h):
        return pl.ds(pl.multiple_of(h * size, 8), size)

    def landing(ref, sem):
        pltpu.make_async_copy(ref, ref, sem).wait()

    def diag_z(k):
        return remote(pieces.at[core, plane, c], pieces.at[core, plane, c], dz_s.at[k], dz_r, col=lax.rem(c + k, n_c))

    def diag_plane(k):
        to = lax.rem(plane + k, planes)
        mine = pieces.at[core, plane]
        return remote(mine, mine, dp_s.at[k], dp_r, row=lax.div(to, n_d) * 2 + core, depth=lax.rem(to, n_d))

    def diag_core():
        return remote(pieces.at[core], pieces.at[core], dc_s, dc_r, row=y * 2 + 1 - core)

    takes = lax.div(c, per)
    goes = (c < last, c > 0, takes != d)
    comes = (c > 0, c < last, takes == d)
    steps = ({"col": c + 1}, {"col": c - 1}, {"depth": 1 - d})

    def raw_copy(way, h):
        span = pl.ds(cuts[h], cuts[h + 1] - cuts[h])
        return remote(raw.at[0, span], raw.at[way + 1, span], raw_s.at[way, h], raw_r.at[way, h], **steps[way])

    def raw_start(ways, hs):
        for h in hs:
            for way in ways:
                pl.when(goes[way])(lambda way=way, h=h: raw_copy(way, h).start())

    def first(i):
        p, q, k, to, lo, skip, count = parts[i]
        src, dst = raw.at[0, pl.ds(lo, count)], wraw.at[k, to, q, pl.ds(skip, count)]
        row, depth = to // n_d * 2 + k, to % n_d
        if p == row * n_c * n_d + depth:
            return False, pltpu.make_async_copy(src, dst, w1_r.at[i])
        return True, remote(src, dst, w1_s.at[i], w1_r.at[i], row=row, col=0, depth=depth)

    def first_start():
        for p in sorted({entry[0] for entry in parts}):
            @pl.when(position == p)
            def _(p=p):
                for i in range(len(parts)):
                    if parts[i][0] == p:
                        first(i)[1].start()

    def first_wait():
        for to in range(planes):
            for k in range(2):
                @pl.when(jnp.logical_and(c == 0, jnp.logical_and(plane == to, core == k)))
                def _(to=to, k=k):
                    for i, (p, q, k_i, to_i, lo, skip, count) in enumerate(parts):
                        if (k_i, to_i) == (k, to):
                            landing(wraw.at[k, to, q, pl.ds(skip, count)], w1_r.at[i])

    middle = jnp.logical_and(c > 0, c < last)
    edge = jnp.logical_not(middle)

    def second(col):
        ref = wraw.at[core, plane] if col < last else wraw.at[core, plane, last]
        return remote(ref, ref, w2_s.at[col], w2_r, col=col)

    def second_all(act):
        @pl.when(c == 0)
        def _():
            for col in [*range(last - 1, 0, -1), last]:
                act(second(col))

    turn = [jnp.where(c > last - c, q, last - q) for q in range(n_c)]

    def third(k, q):
        to = lax.rem(plane + k, planes)
        ref = wraw.at[core, plane, q]
        return remote(
            ref, ref, w3_s.at[k, q], w3_r.at[plane, q], row=lax.div(to, n_d) * 2 + core, depth=lax.rem(to, n_d)
        )

    def third_all(act):
        @pl.when(middle)
        def _():
            for q in turn:
                for k in range(1, planes):
                    act(third(k, q))

        @pl.when(edge)
        def _():
            for k in range(1, planes):
                act(third(k, c))

    def third_start():
        pl.when(middle)(lambda: landing(wraw.at[core, plane], w2_r))
        pl.when(c == last)(lambda: landing(wraw.at[core, plane, last], w2_r))
        third_all(lambda copy: copy.start())
        raw_start((2,), range(1, len(cuts) - 1))

    def fourth(q):
        ref = wraw.at[core, pl.ds(0, planes), q]
        return remote(ref, ref, w4_s.at[q], w4_r.at[q], row=y * 2 + 1 - core)

    def fourth_start():
        def pass_on(q):
            for to in range(planes):
                pl.when(plane != to)(lambda to=to: landing(wraw.at[core, to, q], w3_r.at[to, q]))
            fourth(q).start()

        @pl.when(middle)
        def _():
            for q in turn:
                pass_on(q)

        pl.when(edge)(lambda: pass_on(c))

    def fourth_wait(q):
        landing(wraw.at[1 - core, pl.ds(0, planes), q], w4_r.at[q])

    keep = pltpu.make_async_copy(diag_ref, pieces.at[core, plane, c], piece_s)
    keep.start()
    load = pltpu.make_async_copy(panel, raw.at[0], own_s)
    load.start()
    fetch = pltpu.make_async_copy(trailing, trail, trail_s)
    fetch.start()
    gate = pltpu.get_barrier_semaphore()
    ring = n_c * n_d
    for k in range(1, ring):
        to = lax.rem(c * n_d + d + k, ring)
        pl.semaphore_signal(
            gate, inc=1, device_id={"row": r, "col": lax.div(to, n_d), "depth": lax.rem(to, n_d)},
            device_id_type=pl.DeviceIdType.MESH,
        )
    for k in range(1, n_r * n_d):
        to = lax.rem(r * n_d + d + k, n_r * n_d)
        far = lax.div(to, n_d) != r
        pl.when(far)(lambda to=to: pl.semaphore_signal(
            gate, inc=1, device_id={"row": lax.div(to, n_d), "col": c, "depth": lax.rem(to, n_d)},
            device_id_type=pl.DeviceIdType.MESH,
        ))
    pl.semaphore_wait(gate, ring - 1 + (n_r - 1) * n_d)
    keep.wait()
    for k in range(1, n_c):
        diag_z(k).start()
    load.wait()
    first_start()
    raw_start((0, 1), range(1))
    pl.when(c > 0)(lambda: raw_start((0, 1), range(1, len(cuts) - 1)))
    landing(pieces.at[core, plane, pl.ds(0, n_c - 1)], dz_r)
    for k in range(1, planes):
        diag_plane(k).start()
    first_wait()
    second_all(lambda copy: copy.start())
    pl.when(c == 0)(lambda: raw_start((0, 1), range(1, len(cuts) - 1)))
    raw_start((2,), range(1))
    landing(pieces.at[core, pl.ds(0, planes - 1)], dp_r)
    diag_core().start()
    landing(pieces.at[1 - core], dc_r)
    mine = diag_ref.shape[0]
    for p in range(total):
        p_r, p_c, p_d = p // (n_c * n_d), p // n_d % n_c, p % n_d
        work[p * mine : (p + 1) * mine, :] = pieces[p_r % 2, p_r // 2 * n_d + p_d, p_c]

    stages = {2: third_start, 6: fourth_start}

    def between(k, later):
        for point, action in stages.items():
            if point % 2 == later:
                pl.when(k == point // 2)(action)

    factor_all(work, low, inv, between)

    flip = c > last - c
    v_c = jnp.where(flip, last - c, c)
    v_d = jnp.where(flip, 1 - d, d)

    def task(k):
        end = v_c == 0
        slot = jnp.where(end, 2, jnp.where(k == 1, 2, jnp.where(k == 3, 2 - v_d, 1)))
        col = jnp.where(end, 0, jnp.where(k == 0, 3, jnp.where(k == 1, 0, jnp.where(k == 2, 2, 1))))
        deep = jnp.where(end, 0, jnp.where(k == 1, 1, jnp.where(k == 3, 1 - v_d, 0)))
        j = jnp.where(end, 3, v_d)
        active = jnp.logical_or(v_c == 1, jnp.logical_and(v_d == 1, k == 0))
        return (
            active,
            jnp.where(flip, 3 - slot, slot),
            jnp.where(flip, last - col, col),
            jnp.where(flip, 1 - deep, deep),
            jnp.where(flip, 3 - j, j),
        )

    def prod_copy(t):
        k, h = lax.rem(t, 4), lax.div(t, 4)
        active, slot, col, deep, j = task(k)
        return active, remote(sent.at[k, at(h)], landed.at[j, at(h)], prod_s.at[k, h], prod_r.at[j, h], col=col, depth=deep)

    def launch(t):
        active, copy = prod_copy(t)
        pl.when(active)(lambda: copy.start())

    dense[...] = dot(inv[...], inv[...], 0, 0)
    for h, way in raw_halves[0]:
        pl.when(comes[way])(lambda way=way, h=h: raw_copy(way, h).wait_recv())

    def produce(t, carry):
        k, h = lax.rem(t, 4), lax.div(t, 4)
        active, slot, col, deep, j = task(k)

        @pl.when(jnp.logical_and(h == 0, jnp.logical_or(middle, k == 0)))
        def _():
            fourth_wait(col)
            mult[col] = dot(wraw[:, :, col].reshape(mult.shape[1:]), dense[...], 1, 0)

        @pl.when(t == 4)
        def _():
            for h, way in raw_halves[1]:
                pl.when(comes[way])(lambda way=way, h=h: raw_copy(way, h).wait_recv())

        @pl.when(active)
        def _():
            sent[k, at(h), :] = dot(raw[slot, at(h), :], mult[col], 1, 1)

        pl.when(t > 0)(lambda: launch(t - 1))
        return carry

    lax.fori_loop(0, 4 * split, produce, 0)

    def local(j):
        cj, dj = d * per + lax.div(j, n_d), lax.rem(j, n_d)
        same = dj == d
        slot = jnp.where(cj == c, jnp.where(same, 0, 3), jnp.where(cj < c, 1, 2))
        close = jnp.logical_and(cj - c < 2, c - cj < 2)
        return jnp.logical_or(cj == c, jnp.logical_and(same, close)), slot

    def spot(t):
        return pl.ds(pl.multiple_of(t * size, 8), size)

    def own_rows(h, carry):
        solved[at(h), :] = dot(raw[0, at(h), :], inv[...], 1, 1)
        return carry

    lax.fori_loop(0, split, own_rows, 0)
    launch(4 * split - 1)
    fetch.wait()
    for h in range(len(cuts) - 1):
        pl.when(comes[2])(lambda h=h: raw_copy(2, h).wait_recv())

    def consume(t, carry):
        j, h = lax.div(t, split), lax.rem(t, split)
        here, slot = local(j)

        @pl.when(here)
        def _():
            trail[spot(t), :] = trail[spot(t), :] - dot(raw[slot, at(h), :], mult[c], 1, 1)

        return carry

    lax.fori_loop(0, 4 * split, consume, 0)

    def receive(i, carry):
        h, j = lax.div(i, 4), lax.rem(i, 4)
        t = j * split + h
        here, slot = local(j)

        @pl.when(jnp.logical_not(here))
        def _():
            landing(landed.at[j, at(h)], prod_r.at[j, h])
            trail[spot(t), :] = trail[spot(t), :] - landed[j, at(h), :]

        return carry

    lax.fori_loop(0, 4 * split, receive, 0)
    own[...] = low[pl.ds(pl.multiple_of(position * mine, 8), mine), :]

    for k in range(1, n_c):
        diag_z(k).wait_send()
    for k in range(1, planes):
        diag_plane(k).wait_send()
    diag_core().wait_send()
    for h in range(len(cuts) - 1):
        for way in range(3):
            pl.when(goes[way])(lambda way=way, h=h: raw_copy(way, h).wait_send())
    for p in sorted({entry[0] for entry in parts}):
        @pl.when(position == p)
        def _(p=p):
            for i in range(len(parts)):
                if parts[i][0] == p:
                    far, copy = first(i)
                    if far:
                        copy.wait_send()

    second_all(lambda copy: copy.wait_send())

    third_all(lambda copy: copy.wait_send())

    @pl.when(middle)
    def _():
        for q in range(n_c):
            fourth(q).wait_send()

    pl.when(edge)(lambda: fourth(c).wait_send())

    def drain(t, carry):
        active, copy = prod_copy(t)
        pl.when(active)(lambda: copy.wait_send())
        return carry

    lax.fori_loop(0, 4 * split, drain, 0)


def place(own, solved, updated, own_out, solved_out, updated_out, sems):
    copies = [
        pltpu.make_async_copy(src, dst, sems.at[i])
        for i, (src, dst) in enumerate(((updated, updated_out), (solved, solved_out), (own, own_out)))
    ]
    for copy in copies:
        copy.start()
    for copy in copies:
        copy.wait()


def place_call(*arrays):
    anywhere = pl.BlockSpec(memory_space=pl.ANY)
    return pl.pallas_call(
        place,
        out_shape=tuple(jax.ShapeDtypeStruct(x.shape, x.dtype) for x in arrays),
        in_specs=[anywhere] * 3,
        out_specs=(anywhere,) * 3,
        scratch_shapes=[pltpu.SemaphoreType.DMA((3,))],
        compiler_params=pltpu.CompilerParams(vmem_limit_bytes=1000000),
    )(*arrays)


def near_call(sizes, diag_block, panel, trailing):
    n_r, n_c, n_d = sizes
    mine, n = diag_block.shape
    rows, width = panel.shape
    columns = trailing.shape[1]
    split = 2
    planes = n_r // 2 * n_d
    piece = columns // (2 * planes)
    parts = []
    for to in range(planes - 1, -1, -1):
        for k in range(2):
            for q in range(n_c):
                start = q * columns + (k * planes + to) * piece
                for p in range(start // rows, (start + piece - 1) // rows + 1):
                    lo, hi = max(start, p * rows), min(start + piece, (p + 1) * rows)
                    parts.append((p, q, k, to, lo - p * rows, lo - start, hi - lo))
    vmem, anywhere = pl.BlockSpec(memory_space=pltpu.VMEM), pl.BlockSpec(memory_space=pl.ANY)
    dma = pltpu.SemaphoreType.DMA
    sems = [
        dma, dma, dma, dma((n_c,)), dma, dma((planes,)), dma, dma, dma, dma((3, 3)), dma((3, 3)),
        dma((len(parts),)), dma((len(parts),)), dma((n_c,)), dma, dma((planes, n_c)), dma((planes, n_c)), dma((n_c,)), dma((n_c,)),
        dma((4, split)), dma((4, split)),
    ]
    square = pltpu.VMEM((n, n), jnp.float32)
    return pl.pallas_call(
        functools.partial(near, sizes, parts, split),
        out_shape=(
            jax.ShapeDtypeStruct((mine, n), jnp.float32),
            jax.ShapeDtypeStruct((rows, width), jnp.float32),
            jax.ShapeDtypeStruct(trailing.shape, jnp.float32),
        ),
        in_specs=[pl.BlockSpec(memory_space=pltpu.HBM)] * 3,
        out_specs=(vmem, vmem, vmem),
        scratch_shapes=[
            pltpu.VMEM((4, rows, width), jnp.float32),
            pltpu.VMEM((2, planes, n_c, piece, width), jnp.float32),
            pltpu.VMEM((n_c, columns, width), jnp.float32),
            pltpu.VMEM((4, rows, columns), jnp.float32),
            pltpu.VMEM((4, rows, columns), jnp.float32),
            pltpu.VMEM((2, planes, n_c, mine, n), jnp.float32),
            square, square, square, square,
            sems,
        ],
        compiler_params=pltpu.CompilerParams(collective_id=0, has_side_effects=True, vmem_limit_bytes=40000000),
    )(*(pltpu.with_memory_space_constraint(x, pltpu.HBM) for x in (diag_block, panel, trailing)))


def body(sizes, diag_block, panel_rows, trailing):
    n_r, n_c, n_d = sizes
    if sizes == (4, 4, 2) and panel_rows.shape[0] % 16 == 0:
        return place_call(*near_call(sizes, diag_block, panel_rows, trailing))
    position = (lax.axis_index("row") * n_c + lax.axis_index("col")) * n_d + lax.axis_index("depth")
    mine = diag_block.shape[0]
    own_rows, win_rows = trailing.shape
    rows, width = panel_rows.shape
    unit = math.gcd(rows, win_rows)
    low, weight, solved, held = exchange_call(
        sizes, diag_block, panel_rows.reshape(rows // unit, unit, width), win_rows // unit
    )
    own_factor = lax.dynamic_slice_in_dim(low, position * mine, mine, 0)
    updated = update_call(held.reshape(2 * n_c * rows, width), weight, trailing)
    return (own_factor, solved, updated)


def solution(mesh):
    sizes = tuple(mesh.shape[axis] for axis in AXES)
    specs = (P(AXES, None), P(AXES, None), P(("row", "depth"), "col"))
    return jax.shard_map(
        functools.partial(body, sizes), mesh=mesh, in_specs=specs, out_specs=specs, check_vma=False
    )
```

```python
import functools
import math

import jax
import jax.numpy as jnp
from jax import lax
from jax.experimental import pallas as pl
from jax.experimental.pallas import tpu as pltpu
from jax.sharding import PartitionSpec as P

highest = lax.Precision.HIGHEST
AXES = ("row", "col", "depth")
LANES = 128


def dot(left, right, left_dim, right_dim):
    return lax.dot_general(
        left, right, (((left_dim,), (right_dim,)), ((), ())), precision=highest, preferred_element_type=jnp.float32
    )


def factor_block(block, halfway=None):
    size = block.shape[0]
    step = 8
    lane = lax.broadcasted_iota(jnp.int32, (step, size), 1)
    sub = lax.broadcasted_iota(jnp.int32, (step, size), 0)
    tiles = [block[step * i : step * (i + 1), :] for i in range(size // step)]

    def across(tile, j):
        return jnp.broadcast_to(tile[:, j : j + 1], (step, size))

    def down(tile, s):
        return jnp.broadcast_to(tile[s : s + 1, :], (step, size))

    for t in range(size // step):
        if halfway is not None and t == size // step // 2:
            halfway()
        first = step * t
        tile = tiles[t]
        top = [across(tile, first + k) for k in range(step)]
        source, ratio = [], []
        for s in range(step):
            inverse = 1.0 / down(top[s], s)
            source.append(jnp.where(lane == first + s, 1.0, down(tile, s)) * inverse)
            ratio.append([down(top[k], s) * inverse for k in range(s + 1, step)])
            below = sub > s
            for k in range(s + 1, step):
                top[k] = jnp.where(below, top[k] - top[s] * ratio[s][k - s - 1], top[k])
            tile = jnp.where(below, jnp.where(lane == first + s, 0.0, tile) - top[s] * source[s], tile)
        if t + 1 < size // step:
            total = [jnp.where((lane > first + s) & (lane < first + step), 0.0, source[s]) for s in range(step)]
            for s in range(step - 2, -1, -1):
                for k in range(step - 1, s, -1):
                    total[s] = total[s] - ratio[s][k - s - 1] * total[k]
            panel = (lane >= first) & (lane < first + step)
            for i in range(t + 1, size // step):
                new = jnp.where(panel, 0.0, tiles[i])
                for s in range(step):
                    new = new - across(tiles[i], first + s) * total[s]
                tiles[i] = new
        tiles[t] = tile
    whole = jnp.concatenate(tiles, axis=0)
    r_id = lax.broadcasted_iota(jnp.int32, (size, size), 0)
    c_id = lax.broadcasted_iota(jnp.int32, (size, size), 1)
    pivots = jnp.sum(jnp.where(r_id == c_id, whole, 0.0), axis=1, keepdims=True)
    root = jnp.sqrt(pivots)
    scaled = jnp.where(r_id == c_id, 1.0, whole) / root
    inverse = jnp.where(r_id >= c_id, scaled, 0.0)
    upper = jnp.where(r_id < c_id, scaled, jnp.where(r_id == c_id, root, 0.0))
    return upper.T, inverse


def factor_all(work, low, inv, between=None):
    n = work.shape[0]
    low[...] = jnp.zeros((n, n), jnp.float32)
    inv[...] = jnp.zeros((n, n), jnp.float32)

    def step(k, carry):
        at = pl.ds(pl.multiple_of(k * LANES, LANES), LANES)
        halfway = None if between is None else functools.partial(between, k, 0)
        block_low, block_inv = factor_block(work[at, at], halfway)
        rows = lax.broadcasted_iota(jnp.int32, (n, LANES), 0)
        panel = jnp.where(rows >= (k + 1) * LANES, dot(work[:, at], block_inv, 1, 1), 0.0)
        work[...] = work[...] - dot(panel, panel, 1, 1)
        left = dot(low[at, :], inv[...], 1, 0)
        low[:, at] = panel
        low[at, at] = block_low
        inv[at, :] = -dot(block_inv, left, 1, 0)
        inv[at, at] = block_inv
        if between is not None:
            between(k, 1)
        return carry

    lax.fori_loop(0, n // LANES, step, 0)


def exchange(sizes, cuts, win_units, diag_ref, panel, low, weight, solved, held, window, pieces, work, inv, sems):
    n_r, n_c, n_d = sizes
    total = n_r * n_c * n_d
    half = n_c // 2
    units = panel.shape[0]
    (diag_s, diag_r, ring_s, ring_r, deep_s, deep_r, w1_s, w1_r, w2_s, w2_r, w3_s, w3_r, own_s) = sems
    r, c, d = lax.axis_index("row"), lax.axis_index("col"), lax.axis_index("depth")
    position = (r * n_c + c) * n_d + d

    def remote(src, dst, send, recv, **where):
        return pltpu.make_async_remote_copy(
            src_ref=src,
            dst_ref=dst,
            send_sem=send,
            recv_sem=recv,
            device_id={"row": where.get("row", r), "col": where.get("col", c), "depth": where.get("depth", d)},
            device_id_type=pl.DeviceIdType.MESH,
        )

    def taker(block):
        return lax.div(block * n_d + d, n_c)

    def slot(block):
        return jnp.where(taker(block) == d, block * n_d + d - n_c * d, n_c + block)

    def at(h):
        return pl.ds(cuts[h], cuts[h + 1] - cuts[h])

    def send_diag(k, carry):
        to = lax.rem(position + k, total)
        remote(
            diag_ref, pieces.at[position], diag_s, diag_r,
            row=lax.div(to, n_c * n_d), col=lax.rem(lax.div(to, n_d), n_c), depth=lax.rem(to, n_d),
        ).start()
        return carry

    lax.fori_loop(1, total, send_diag, 0)
    pieces[position] = diag_ref[...]

    def window_parts():
        for p in range(-(-n_c * win_units // units)):
            for b in range(n_c):
                lo, hi = max(b * win_units, p * units), min((b + 1) * win_units, (p + 1) * units)
                if lo < hi:
                    yield p, b, lo, hi - lo

    def part(p, b, lo, count):
        src = panel.at[pl.ds(lo - p * units, count)]
        dst = window.at[pl.ds(lo - b * win_units, count)]
        if p == b * n_d:
            return pltpu.make_async_copy(src, dst, w1_r.at[p])
        return remote(src, dst, w1_s.at[p, b], w1_r.at[p], row=0, col=b, depth=0)

    root = jnp.logical_and(r == 0, d == 0)
    for p, b, lo, count in window_parts():
        @pl.when(position == p)
        def _(p=p, b=b, lo=lo, count=count):
            part(p, b, lo, count).start()

    def to_depth(k):
        return remote(window, window, w2_s.at[k], w2_r, depth=k)

    def to_row(k):
        return remote(window, window, w3_s.at[k], w3_r, row=k)

    def window_second():
        for p, b, lo, count in window_parts():
            @pl.when(jnp.logical_and(root, c == b))
            def _(p=p, b=b, lo=lo, count=count):
                if p == b * n_d:
                    part(p, b, lo, count).wait()
                else:
                    piece = window.at[pl.ds(lo - b * win_units, count)]
                    pltpu.make_async_copy(piece, piece, w1_r.at[p]).wait()

        @pl.when(root)
        def _():
            for k in range(1, n_d):
                to_depth(k).start()

    def window_third():
        @pl.when(jnp.logical_and(r == 0, d != 0))
        def _():
            pltpu.make_async_copy(window, window, w2_r).wait()

        @pl.when(r == 0)
        def _():
            for k in range(1, n_r):
                to_row(k).start()

    def ring(way, s, h):
        block = lax.rem(c + n_c - s + 1, n_c) if way == 0 else lax.rem(c + s - 1, n_c)
        to = lax.rem(c + 1, n_c) if way == 0 else lax.rem(c + n_c - 1, n_c)
        dst = held.at[slot(block), at(h)]
        src = panel.at[at(h)] if s == 1 else dst
        return remote(src, dst, ring_s.at[way, s - 1, h], ring_r.at[way, s - 1, h], col=to)

    def ring_parts(s):
        return [(0, 0), (1, 1)] + ([(0, 1), (1, 0)] if s < half else [])

    def deep(step, h):
        block = lax.rem(c + n_c - step, n_c)
        to = taker(block)
        index = block * n_d + d - n_c * to
        src = panel.at[at(h)] if step == 0 else held.at[slot(block), at(h)]
        where = step + half - 1
        return to, remote(
            src, held.at[index, at(h)], deep_s.at[where, h], deep_r.at[index, h], depth=to
        )

    def start_deep(step, h):
        to, copy = deep(step, h)

        @pl.when(to != d)
        def _():
            copy.start()

    def own_copy():
        return pltpu.make_async_copy(panel, held.at[slot(c)], own_s)

    for way, h in ring_parts(1):
        ring(way, 1, h).start()
    for h in range(2):
        start_deep(0, h)

    @pl.when(taker(c) == d)
    def _():
        own_copy().start()

    def arrived(s, parts):
        for way, h in parts:
            ring(way, s, h).wait_recv()
            if s < half and (s + 1 < half or way == h):
                ring(way, s + 1, h).start()
            step = s if (way == 0 or s == half) else -s
            start_deep(step, h)

    def between(k, later):
        def when(point, action):
            if point % 2 == later:
                pl.when(k == point // 2)(action)

        when(1, window_second)
        when(3, window_third)
        if half > 1:
            when(2, lambda: arrived(1, ring_parts(1)[:2]))
            when(6, lambda: arrived(1, ring_parts(1)[2:]))

    every = pieces.at[pl.ds(0, total - 1)]
    pltpu.make_async_copy(every, every, diag_r).wait()
    mine = diag_ref.shape[0]
    for p in range(total):
        work[p * mine : (p + 1) * mine, :] = pieces[p]
    factor_all(work, low, inv, between)

    @pl.when(r != 0)
    def _():
        pltpu.make_async_copy(window, window, w3_r).wait()

    weight[...] = dot(dot(window[...].reshape(weight.shape), inv[...], 1, 1), inv[...], 1, 0)
    solved[...] = dot(panel[...].reshape(solved.shape), inv[...], 1, 1)
    for s in range(2 if half > 1 else 1, half + 1):
        arrived(s, ring_parts(s))

    for j in range(n_c):
        q = n_c * d + j

        @pl.when(lax.rem(q, n_d) != d)
        def _(j=j):
            for h in range(2):
                landed = held.at[j, at(h)]
                pltpu.make_async_copy(landed, landed, deep_r.at[j, h]).wait()

    pltpu.make_async_copy(every, every, diag_s).wait()
    for s in range(1, half + 1):
        for way, h in ring_parts(s):
            ring(way, s, h).wait_send()
    for step in range(1 - half, half + 1):
        for h in range(2):
            to, copy = deep(step, h)

            @pl.when(to != d)
            def _(copy=copy):
                copy.wait_send()

    @pl.when(taker(c) == d)
    def _():
        own_copy().wait()

    for p, b, lo, count in window_parts():
        if p != b * n_d:
            @pl.when(position == p)
            def _(p=p, b=b, lo=lo, count=count):
                part(p, b, lo, count).wait_send()

    @pl.when(root)
    def _():
        for k in range(1, n_d):
            to_depth(k).wait_send()

    @pl.when(r == 0)
    def _():
        for k in range(1, n_r):
            to_row(k).wait_send()


def exchange_call(sizes, diag_block, panel, win_units):
    n_r, n_c, n_d = sizes
    total = n_r * n_c * n_d
    units, unit, width = panel.shape
    n = diag_block.shape[1]
    square = jax.ShapeDtypeStruct((n, n), jnp.float32)
    vmem, anywhere = pl.BlockSpec(memory_space=pltpu.VMEM), pl.BlockSpec(memory_space=pl.ANY)
    dma, owners = pltpu.SemaphoreType.DMA, -(-n_c * win_units // units)
    sems = [
        dma, dma, dma((2, n_c // 2, 2)), dma((2, n_c // 2, 2)), dma((n_c, 2)), dma((n_c, 2)),
        dma((owners, n_c)), dma((owners,)), dma((n_d,)), dma, dma((n_r,)), dma, dma,
    ]
    return pl.pallas_call(
        functools.partial(exchange, sizes, (0, units // 2, units), win_units),
        out_shape=(
            square,
            jax.ShapeDtypeStruct((win_units * unit, width), jnp.float32),
            jax.ShapeDtypeStruct((units * unit, width), jnp.float32),
            jax.ShapeDtypeStruct((2 * n_c, units, unit, width), jnp.float32),
        ),
        in_specs=[vmem, vmem],
        out_specs=(vmem, vmem, vmem, anywhere),
        scratch_shapes=[
            pltpu.VMEM((win_units, unit, width), jnp.float32),
            pltpu.VMEM((total, diag_block.shape[0], n), jnp.float32),
            pltpu.VMEM((n, n), jnp.float32),
            pltpu.VMEM((n, n), jnp.float32),
            sems,
        ],
        compiler_params=pltpu.CompilerParams(has_side_effects=True),
    )(diag_block, panel)


def update(held, weight, trailing, out):
    out[...] = trailing[...] - dot(held[...], weight[...], 1, 1)


def update_call(held, weight, trailing):
    rows, columns = trailing.shape
    width = held.shape[1]
    chunk = max(m for m in range(8, 1025, 8) if rows % m == 0)
    return pl.pallas_call(
        update,
        grid=(rows // chunk,),
        out_shape=jax.ShapeDtypeStruct(trailing.shape, jnp.float32),
        in_specs=[
            pl.BlockSpec((chunk, width), lambda i: (i, 0)),
            pl.BlockSpec((columns, width), lambda i: (0, 0)),
            pl.BlockSpec((chunk, columns), lambda i: (i, 0)),
        ],
        out_specs=pl.BlockSpec((chunk, columns), lambda i: (i, 0)),
    )(held, weight, trailing)


def near(sizes, parts, split, diag_ref, panel, trailing, own, solved, trail, raw, wraw, mult, sent,
         landed, pieces, work, low, inv, dense, sems):
    n_r, n_c, n_d = sizes
    total = n_r * n_c * n_d
    planes = n_r // 2 * n_d
    last = n_c - 1
    per = n_c // n_d
    rows = raw.shape[1]
    size = rows // split
    sixth = rows // 6
    cuts = (0, sixth, 2 * sixth, 4 * sixth, rows)
    (own_s, trail_s, piece_s, dz_s, dz_r, dp_s, dp_r, dc_s, dc_r, raw_s, raw_r, w1_s, w1_r, w2_s, w2_r, w3_s, w3_r, w4_s, w4_r,
     prod_s, prod_r) = sems
    r, c, d = lax.axis_index("row"), lax.axis_index("col"), lax.axis_index("depth")
    y, core = lax.div(r, 2), lax.rem(r, 2)
    plane = y * n_d + d
    position = (r * n_c + c) * n_d + d

    def remote(src, dst, send, recv, **where):
        return pltpu.make_async_remote_copy(
            src_ref=src,
            dst_ref=dst,
            send_sem=send,
            recv_sem=recv,
            device_id={"row": where.get("row", r), "col": where.get("col", c), "depth": where.get("depth", d)},
            device_id_type=pl.DeviceIdType.MESH,
        )

    def at(h):
        return pl.ds(pl.multiple_of(h * size, 8), size)

    def landing(ref, sem):
        pltpu.make_async_copy(ref, ref, sem).wait()

    def diag_z(k):
        return remote(pieces.at[core, plane, c], pieces.at[core, plane, c], dz_s.at[k], dz_r, col=lax.rem(c + k, n_c))

    def diag_plane(k):
        to = lax.rem(plane + k, planes)
        mine = pieces.at[core, plane]
        return remote(mine, mine, dp_s.at[k], dp_r, row=lax.div(to, n_d) * 2 + core, depth=lax.rem(to, n_d))

    def diag_core():
        return remote(pieces.at[core], pieces.at[core], dc_s, dc_r, row=y * 2 + 1 - core)

    takes = lax.div(c, per)
    goes = (c < last, c > 0, takes != d)
    comes = (c > 0, c < last, takes == d)
    steps = ({"col": c + 1}, {"col": c - 1}, {"depth": 1 - d})

    def raw_copy(way, h):
        span = pl.ds(cuts[h], cuts[h + 1] - cuts[h])
        return remote(raw.at[0, span], raw.at[way + 1, span], raw_s.at[way, h], raw_r.at[way, h], **steps[way])

    def raw_start(ways, hs):
        for h in hs:
            for way in ways:
                pl.when(goes[way])(lambda way=way, h=h: raw_copy(way, h).start())

    def first(i):
        p, q, k, to, lo, skip, count = parts[i]
        src, dst = raw.at[0, pl.ds(lo, count)], wraw.at[k, to, q, pl.ds(skip, count)]
        row, depth = to // n_d * 2 + k, to % n_d
        if p == row * n_c * n_d + depth:
            return False, pltpu.make_async_copy(src, dst, w1_r.at[i])
        return True, remote(src, dst, w1_s.at[i], w1_r.at[i], row=row, col=0, depth=depth)

    def first_start():
        for p in sorted({entry[0] for entry in parts}):
            @pl.when(position == p)
            def _(p=p):
                for i in range(len(parts)):
                    if parts[i][0] == p:
                        first(i)[1].start()

    def first_wait():
        for to in range(planes):
            for k in range(2):
                @pl.when(jnp.logical_and(c == 0, jnp.logical_and(plane == to, core == k)))
                def _(to=to, k=k):
                    for i, (p, q, k_i, to_i, lo, skip, count) in enumerate(parts):
                        if (k_i, to_i) == (k, to):
                            landing(wraw.at[k, to, q, pl.ds(skip, count)], w1_r.at[i])

    middle = jnp.logical_and(c > 0, c < last)
    edge = jnp.logical_not(middle)

    def second(col):
        ref = wraw.at[core, plane] if col < last else wraw.at[core, plane, last]
        return remote(ref, ref, w2_s.at[col], w2_r, col=col)

    def second_all(act):
        @pl.when(c == 0)
        def _():
            for col in [*range(last - 1, 0, -1), last]:
                act(second(col))

    turn = [jnp.where(c > last - c, q, last - q) for q in range(n_c)]

    def third(k, q):
        to = lax.rem(plane + k, planes)
        ref = wraw.at[core, plane, q]
        return remote(
            ref, ref, w3_s.at[k, q], w3_r.at[plane, q], row=lax.div(to, n_d) * 2 + core, depth=lax.rem(to, n_d)
        )

    def third_all(act):
        @pl.when(middle)
        def _():
            for q in turn:
                for k in range(1, planes):
                    act(third(k, q))

        @pl.when(edge)
        def _():
            for k in range(1, planes):
                act(third(k, c))

    def third_start():
        pl.when(middle)(lambda: landing(wraw.at[core, plane], w2_r))
        pl.when(c == last)(lambda: landing(wraw.at[core, plane, last], w2_r))
        third_all(lambda copy: copy.start())
        raw_start((2,), range(1, len(cuts) - 1))

    def fourth(q):
        ref = wraw.at[core, pl.ds(0, planes), q]
        return remote(ref, ref, w4_s.at[q], w4_r.at[q], row=y * 2 + 1 - core)

    def fourth_start():
        def pass_on(q):
            for to in range(planes):
                pl.when(plane != to)(lambda to=to: landing(wraw.at[core, to, q], w3_r.at[to, q]))
            fourth(q).start()

        @pl.when(middle)
        def _():
            for q in turn:
                pass_on(q)

        pl.when(edge)(lambda: pass_on(c))

    def fourth_wait(q):
        landing(wraw.at[1 - core, pl.ds(0, planes), q], w4_r.at[q])

    keep = pltpu.make_async_copy(diag_ref, pieces.at[core, plane, c], piece_s)
    keep.start()
    load = pltpu.make_async_copy(panel, raw.at[0], own_s)
    load.start()
    fetch = pltpu.make_async_copy(trailing, trail, trail_s)
    fetch.start()
    gate = pltpu.get_barrier_semaphore()
    ring = n_c * n_d
    for k in range(1, ring):
        to = lax.rem(c * n_d + d + k, ring)
        pl.semaphore_signal(
            gate, inc=1, device_id={"row": r, "col": lax.div(to, n_d), "depth": lax.rem(to, n_d)},
            device_id_type=pl.DeviceIdType.MESH,
        )
    for k in range(1, n_r * n_d):
        to = lax.rem(r * n_d + d + k, n_r * n_d)
        far = lax.div(to, n_d) != r
        pl.when(far)(lambda to=to: pl.semaphore_signal(
            gate, inc=1, device_id={"row": lax.div(to, n_d), "col": c, "depth": lax.rem(to, n_d)},
            device_id_type=pl.DeviceIdType.MESH,
        ))
    pl.semaphore_wait(gate, ring - 1 + (n_r - 1) * n_d)
    keep.wait()
    for k in range(1, n_c):
        diag_z(k).start()
    load.wait()
    first_start()
    raw_start((0, 1), range(1))
    pl.when(c > 0)(lambda: raw_start((0, 1), range(1, len(cuts) - 1)))
    landing(pieces.at[core, plane, pl.ds(0, n_c - 1)], dz_r)
    for k in range(1, planes):
        diag_plane(k).start()
    first_wait()
    second_all(lambda copy: copy.start())
    pl.when(c == 0)(lambda: raw_start((0, 1), range(1, len(cuts) - 1)))
    raw_start((2,), range(1))
    landing(pieces.at[core, pl.ds(0, planes - 1)], dp_r)
    diag_core().start()
    landing(pieces.at[1 - core], dc_r)
    mine = diag_ref.shape[0]
    for p in range(total):
        p_r, p_c, p_d = p // (n_c * n_d), p // n_d % n_c, p % n_d
        work[p * mine : (p + 1) * mine, :] = pieces[p_r % 2, p_r // 2 * n_d + p_d, p_c]

    stages = {2: third_start, 6: fourth_start}

    def between(k, later):
        for point, action in stages.items():
            if point % 2 == later:
                pl.when(k == point // 2)(action)

    factor_all(work, low, inv, between)

    flip = c > last - c
    v_c = jnp.where(flip, last - c, c)
    v_d = jnp.where(flip, 1 - d, d)

    def task(k):
        end = v_c == 0
        slot = jnp.where(end, 2, jnp.where(k == 1, 2, jnp.where(k == 3, 2 - v_d, 1)))
        col = jnp.where(end, 0, jnp.where(k == 0, 3, jnp.where(k == 1, 0, jnp.where(k == 2, 2, 1))))
        deep = jnp.where(end, 0, jnp.where(k == 1, 1, jnp.where(k == 3, 1 - v_d, 0)))
        j = jnp.where(end, 3, v_d)
        active = jnp.logical_or(v_c == 1, jnp.logical_and(v_d == 1, k == 0))
        return (
            active,
            jnp.where(flip, 3 - slot, slot),
            jnp.where(flip, last - col, col),
            jnp.where(flip, 1 - deep, deep),
            jnp.where(flip, 3 - j, j),
        )

    def prod_copy(t):
        k, h = lax.rem(t, 4), lax.div(t, 4)
        active, slot, col, deep, j = task(k)
        return active, remote(sent.at[k, at(h)], landed.at[j, at(h)], prod_s.at[k, h], prod_r.at[j, h], col=col, depth=deep)

    def launch(t):
        active, copy = prod_copy(t)
        pl.when(active)(lambda: copy.start())

    dense[...] = dot(inv[...], inv[...], 0, 0)
    def raw_wait(now):
        for i in range(len(cuts) - 1):
            if cuts[i] // size == now:
                for way in range(2):
                    pl.when(comes[way])(lambda way=way, i=i: raw_copy(way, i).wait_recv())

    def produce(t, carry):
        k, h = lax.rem(t, 4), lax.div(t, 4)
        active, slot, col, deep, j = task(k)

        @pl.when(jnp.logical_and(h == 0, jnp.logical_or(middle, k == 0)))
        def _():
            fourth_wait(col)
            mult[col] = dot(wraw[:, :, col].reshape(mult.shape[1:]), dense[...], 1, 0)

        for now in range(split):
            pl.when(t == 4 * now)(lambda now=now: raw_wait(now))

        @pl.when(active)
        def _():
            sent[k, at(h), :] = dot(raw[slot, at(h), :], mult[col], 1, 1)

        pl.when(t > 0)(lambda: launch(t - 1))
        return carry

    lax.fori_loop(0, 4 * split, produce, 0)

    def local(j):
        cj, dj = d * per + lax.div(j, n_d), lax.rem(j, n_d)
        same = dj == d
        slot = jnp.where(cj == c, jnp.where(same, 0, 3), jnp.where(cj < c, 1, 2))
        close = jnp.logical_and(cj - c < 2, c - cj < 2)
        return jnp.logical_or(cj == c, jnp.logical_and(same, close)), slot

    def spot(t):
        return pl.ds(pl.multiple_of(t * size, 8), size)

    def own_rows(h, carry):
        solved[at(h), :] = dot(raw[0, at(h), :], inv[...], 1, 1)
        return carry

    lax.fori_loop(0, split, own_rows, 0)
    launch(4 * split - 1)
    fetch.wait()
    for h in range(len(cuts) - 1):
        pl.when(comes[2])(lambda h=h: raw_copy(2, h).wait_recv())

    def consume(t, carry):
        j, h = lax.div(t, split), lax.rem(t, split)
        here, slot = local(j)

        @pl.when(here)
        def _():
            trail[spot(t), :] = trail[spot(t), :] - dot(raw[slot, at(h), :], mult[c], 1, 1)

        return carry

    lax.fori_loop(0, 4 * split, consume, 0)

    def receive(i, carry):
        h, j = lax.div(i, 4), lax.rem(i, 4)
        t = j * split + h
        here, slot = local(j)

        @pl.when(jnp.logical_not(here))
        def _():
            landing(landed.at[j, at(h)], prod_r.at[j, h])
            trail[spot(t), :] = trail[spot(t), :] - landed[j, at(h), :]

        return carry

    lax.fori_loop(0, 4 * split, receive, 0)
    own[...] = low[pl.ds(pl.multiple_of(position * mine, 8), mine), :]

    for k in range(1, n_c):
        diag_z(k).wait_send()
    for k in range(1, planes):
        diag_plane(k).wait_send()
    diag_core().wait_send()
    for h in range(len(cuts) - 1):
        for way in range(3):
            pl.when(goes[way])(lambda way=way, h=h: raw_copy(way, h).wait_send())
    for p in sorted({entry[0] for entry in parts}):
        @pl.when(position == p)
        def _(p=p):
            for i in range(len(parts)):
                if parts[i][0] == p:
                    far, copy = first(i)
                    if far:
                        copy.wait_send()

    second_all(lambda copy: copy.wait_send())

    third_all(lambda copy: copy.wait_send())

    @pl.when(middle)
    def _():
        for q in range(n_c):
            fourth(q).wait_send()

    pl.when(edge)(lambda: fourth(c).wait_send())

    def drain(t, carry):
        active, copy = prod_copy(t)
        pl.when(active)(lambda: copy.wait_send())
        return carry

    lax.fori_loop(0, 4 * split, drain, 0)


def place(own, solved, updated, own_out, solved_out, updated_out, sems):
    copies = [
        pltpu.make_async_copy(src, dst, sems.at[i])
        for i, (src, dst) in enumerate(((updated, updated_out), (solved, solved_out), (own, own_out)))
    ]
    for copy in copies:
        copy.start()
    for copy in copies:
        copy.wait()


def place_call(*arrays):
    anywhere = pl.BlockSpec(memory_space=pl.ANY)
    return pl.pallas_call(
        place,
        out_shape=tuple(jax.ShapeDtypeStruct(x.shape, x.dtype) for x in arrays),
        in_specs=[anywhere] * 3,
        out_specs=(anywhere,) * 3,
        scratch_shapes=[pltpu.SemaphoreType.DMA((3,))],
        compiler_params=pltpu.CompilerParams(vmem_limit_bytes=1000000),
    )(*arrays)


def near_call(sizes, diag_block, panel, trailing):
    n_r, n_c, n_d = sizes
    mine, n = diag_block.shape
    rows, width = panel.shape
    columns = trailing.shape[1]
    split = 3
    planes = n_r // 2 * n_d
    piece = columns // (2 * planes)
    parts = []
    for to in range(planes - 1, -1, -1):
        for k in range(2):
            for q in range(n_c):
                start = q * columns + (k * planes + to) * piece
                for p in range(start // rows, (start + piece - 1) // rows + 1):
                    lo, hi = max(start, p * rows), min(start + piece, (p + 1) * rows)
                    parts.append((p, q, k, to, lo - p * rows, lo - start, hi - lo))
    vmem, anywhere = pl.BlockSpec(memory_space=pltpu.VMEM), pl.BlockSpec(memory_space=pl.ANY)
    dma = pltpu.SemaphoreType.DMA
    sems = [
        dma, dma, dma, dma((n_c,)), dma, dma((planes,)), dma, dma, dma, dma((3, 4)), dma((3, 4)),
        dma((len(parts),)), dma((len(parts),)), dma((n_c,)), dma, dma((planes, n_c)), dma((planes, n_c)), dma((n_c,)), dma((n_c,)),
        dma((4, split)), dma((4, split)),
    ]
    square = pltpu.VMEM((n, n), jnp.float32)
    return pl.pallas_call(
        functools.partial(near, sizes, parts, split),
        out_shape=(
            jax.ShapeDtypeStruct((mine, n), jnp.float32),
            jax.ShapeDtypeStruct((rows, width), jnp.float32),
            jax.ShapeDtypeStruct(trailing.shape, jnp.float32),
        ),
        in_specs=[pl.BlockSpec(memory_space=pltpu.HBM)] * 3,
        out_specs=(vmem, vmem, vmem),
        scratch_shapes=[
            pltpu.VMEM((4, rows, width), jnp.float32),
            pltpu.VMEM((2, planes, n_c, piece, width), jnp.float32),
            pltpu.VMEM((n_c, columns, width), jnp.float32),
            pltpu.VMEM((4, rows, columns), jnp.float32),
            pltpu.VMEM((4, rows, columns), jnp.float32),
            pltpu.VMEM((2, planes, n_c, mine, n), jnp.float32),
            square, square, square, square,
            sems,
        ],
        compiler_params=pltpu.CompilerParams(collective_id=0, has_side_effects=True, vmem_limit_bytes=40000000),
    )(*(pltpu.with_memory_space_constraint(x, pltpu.HBM) for x in (diag_block, panel, trailing)))


def body(sizes, diag_block, panel_rows, trailing):
    n_r, n_c, n_d = sizes
    if sizes == (4, 4, 2) and panel_rows.shape[0] % 48 == 0:
        return place_call(*near_call(sizes, diag_block, panel_rows, trailing))
    position = (lax.axis_index("row") * n_c + lax.axis_index("col")) * n_d + lax.axis_index("depth")
    mine = diag_block.shape[0]
    own_rows, win_rows = trailing.shape
    rows, width = panel_rows.shape
    unit = math.gcd(rows, win_rows)
    low, weight, solved, held = exchange_call(
        sizes, diag_block, panel_rows.reshape(rows // unit, unit, width), win_rows // unit
    )
    own_factor = lax.dynamic_slice_in_dim(low, position * mine, mine, 0)
    updated = update_call(held.reshape(2 * n_c * rows, width), weight, trailing)
    return (own_factor, solved, updated)


def solution(mesh):
    sizes = tuple(mesh.shape[axis] for axis in AXES)
    specs = (P(AXES, None), P(AXES, None), P(("row", "depth"), "col"))
    return jax.shard_map(
        functools.partial(body, sizes), mesh=mesh, in_specs=specs, out_specs=specs, check_vma=False
    )
```
